128 devices in a mesh: band: 128 (over z, y, x, core).
Axes of the slice: x: 4, y: 4, z: 4, core: 2. Of those that a mesh axis runs over, the one named last changes fastest.
Arguments:
- orbitals: float32 [128, 64, 4096], P('band'), may hold values from -6 to 6
- kernel_values: float32 [32], replicated, may hold values from 0.2 to 4
- shell_index: int32 [64, 4096], replicated, may hold values from 0 to 31, as said below
Outputs:
- exchange_term: float32 [128, 64, 4096], P('band')
- margin: float32 [128, 128], P('band')
The draws below stay inside these ranges and needn't reach their ends.
Inputs may be any that keep to these rules, and one draw needn't show every extreme that they name: `shell_index`: the class of a wave vector is unchanged when any one of its indices a is replaced by (64 - a) mod 64.
All inputs are finite; a program needn't handle non-finite values.
Results may differ from the reference program's by a relative error of at most 0.0003.
Values sent between devices are 32-bit elements; how exact they have to be, the bound alone decides.
A program may use at most 64 MiB of HBM per device.

```python
import math
import jax
import jax.numpy as jnp
from jax import lax

GRID = 64
NSHELL = 32
NBD = 1
STEPS = 2
BANDS = 128
N_BAND = 128


def draw_shell_index(key, part):
    half_count = GRID // 2 + 1
    classes = jax.random.randint(key, (half_count, half_count, half_count), 0, NSHELL)
    positions = jnp.arange(GRID, dtype=jnp.int32)
    mirrored = jnp.minimum(positions, GRID - positions)
    whole_grid = classes[mirrored][:, mirrored][:, :, mirrored]
    return whole_grid.reshape(GRID, GRID * GRID).astype(jnp.int32)


def block_levels(rng, dims, shards, smallest, largest):
    loudness = 1.0
    for axis_at, parts in shards:
        draws = jax.random.uniform(jax.random.fold_in(jax.random.fold_in(rng, 6), axis_at), (parts,), jnp.float32, smallest / len(shards), largest / len(shards))
        loudness = loudness * jnp.repeat(jnp.exp(draws), dims[axis_at] // parts).reshape((-1,) + (1,) * (len(dims) - 1 - axis_at))
    return loudness


def normal_values(key, shape, spread, reach, cuts=(), kind=jnp.bfloat16):
    result = jax.random.normal(key, shape, jnp.float32) * spread
    if len(cuts) > 0:
        result = block_levels(key, shape, cuts, -0.22, 0.18) * result
    return jnp.clip(result, min=-reach, max=reach).astype(kind)


def setup_inputs(seed: int = 0) -> dict:
    keys = jax.random.split(jax.random.key(seed), 4)
    orbitals = normal_values(keys[0], (BANDS, GRID, GRID * GRID), 1.0, 6.0, ((0, 128),), jnp.float32)
    kernel_values = jnp.clip(jnp.exp(jax.random.uniform(keys[1], (NSHELL,), jnp.float32, math.log(0.2), math.log(4.0))), 0.2, 4.0)
    shell_index = draw_shell_index(jax.random.fold_in(keys[3], 71), 0)
    return dict(orbitals=orbitals, kernel_values=kernel_values, shell_index=shell_index)


def reference(orbitals, kernel_values, shell_index):
    volume = GRID ** 3
    kernel = kernel_values[shell_index].reshape(GRID, GRID, GRID)[:, :, : GRID // 2 + 1]
    orbital_cubes = orbitals.reshape(BANDS, GRID, GRID, GRID)

    def block_term(block_index):
        shifts = jnp.arange(-STEPS, STEPS + 1, dtype=jnp.int32)
        partner_blocks = (block_index + shifts) % N_BAND
        band_rows = (partner_blocks[:, None] * NBD + jnp.arange(NBD, dtype=jnp.int32)[None]).reshape(-1)
        partners = jnp.take(orbital_cubes, band_rows, axis=0)
        own_bands = lax.dynamic_slice_in_dim(orbital_cubes, (block_index * NBD).astype(jnp.int32), NBD, 0)

        def one_orbital(single):
            density = single[None] * partners
            spectrum = jnp.fft.rfftn(density, axes=(1, 2, 3)) * kernel[None]
            potential = jnp.fft.irfftn(spectrum, s=(GRID, GRID, GRID), axes=(1, 2, 3))
            return -jnp.sum(potential * partners, axis=0)

        return lax.map(one_orbital, own_bands)

    exchange_terms = lax.map(block_term, jnp.arange(N_BAND, dtype=jnp.int32))
    exchange_terms = exchange_terms.reshape(BANDS, GRID, GRID * GRID)
    margin = jnp.dot(orbitals.reshape(BANDS, volume), exchange_terms.reshape(BANDS, volume).T,
                      precision=lax.Precision.HIGHEST, preferred_element_type=jnp.float32) / volume
    return exchange_terms, margin
```

```python
import math

import jax
import jax.numpy as jnp
import numpy as np
from jax import lax
from jax.experimental import pallas as pl
from jax.experimental.pallas import tpu as pltpu
from jax.sharding import PartitionSpec as P

GRID = 64
WIDE = GRID * GRID
BANDS = 128
TILES = 16
TILED = (8, 32, 8, 128)
MESH = pl.DeviceIdType.MESH
f32 = jnp.float32
bf16 = jnp.bfloat16


def cas(angle):
    return math.cos(angle) + math.sin(angle)


def cas_table():
    index = np.arange(GRID)
    angle = 2.0 * math.pi / GRID * (index[:, None] * index[None] % GRID)
    return np.cos(angle) + np.sin(angle)


def frequencies(k):
    return (0, 32, 16, 48) if k == 0 else (k, 32 - k, 64 - k, 32 + k)


def mixing(k):
    table = np.zeros((4, 4))
    for t, b in enumerate(frequencies(k)):
        for q in range(4):
            part, r = q // 2, q % 2
            angle = 2.0 * math.pi * b * r / GRID
            if k == 0:
                table[q, t] = cas(angle) if (part == 0) == (b % 32 == 0) else 0.0
            elif part == 0:
                table[q, t] = cas(angle)
            else:
                sign = 1.0 if b in (k, 32 + k) else -1.0
                table[q, t] = sign * (math.sin(angle) - math.cos(angle))
    return table


def constants():
    table = cas_table()
    high = table.astype(np.float32).astype(bf16)
    low = (table - high.astype(np.float64)).astype(np.float32).astype(bf16)
    left = np.concatenate([high, low, high], axis=1)
    four = np.tile(table, (1, 4)).astype(np.float32)
    mixes = np.stack([mixing(k) for k in range(TILES)])
    forward = np.repeat(mixes.reshape(TILES * 4, 4), GRID, axis=1).astype(np.float32)
    backward = np.repeat(
        np.swapaxes(mixes, 1, 2).reshape(TILES * 4, 4), GRID, axis=1
    ).astype(np.float32)
    return left, four, forward, backward


def half_spectrum(xs):
    n = len(xs)
    if n == 2:
        return [xs[0] + xs[1], xs[0] - xs[1]], [None, None]
    even_re, even_im = half_spectrum(xs[0::2])
    odd_re, odd_im = half_spectrum(xs[1::2])
    h, q = n // 2, n // 4
    re, im = [None] * (h + 1), [None] * (h + 1)
    re[0], re[h] = even_re[0] + odd_re[0], even_re[0] - odd_re[0]
    for k in range(1, q):
        c, s = math.cos(2 * math.pi * k / n), -math.sin(2 * math.pi * k / n)
        if 2 * k == q:
            t_re, t_im = (odd_re[k] + odd_im[k]) * c, (odd_im[k] - odd_re[k]) * c
        else:
            t_re = odd_re[k] * c - odd_im[k] * s
            t_im = odd_re[k] * s + odd_im[k] * c
        re[k], im[k] = even_re[k] + t_re, even_im[k] + t_im
        re[h - k], im[h - k] = even_re[k] - t_re, t_im - even_im[k]
    re[q], im[q] = even_re[q], -odd_re[q]
    return re, im


def half_spectrum_transposed(re, im):
    h = len(re) - 1
    n = 2 * h
    if n == 2:
        return [re[0] + re[1], re[0] - re[1]]
    q = n // 4
    even_re, even_im = [None] * (q + 1), [None] * (q + 1)
    odd_re, odd_im = [None] * (q + 1), [None] * (q + 1)
    even_re[0], odd_re[0] = re[0] + re[h], re[0] - re[h]
    for k in range(1, q):
        even_re[k], even_im[k] = re[k] + re[h - k], im[k] - im[h - k]
        d_re, d_im = re[k] - re[h - k], im[k] + im[h - k]
        c, s = math.cos(2 * math.pi * k / n), math.sin(2 * math.pi * k / n)
        if 2 * k == q:
            odd_re[k], odd_im[k] = (d_re - d_im) * c, (d_re + d_im) * c
        else:
            odd_re[k], odd_im[k] = d_re * c - d_im * s, d_re * s + d_im * c
    even_re[q], odd_re[q] = re[q], -im[q]
    out = [None] * n
    out[0::2] = half_spectrum_transposed(even_re, even_im)
    out[1::2] = half_spectrum_transposed(odd_re, odd_im)
    return out


def split(x):
    high = x.astype(bf16)
    return high, (x - high.astype(f32)).astype(bf16)


def dot(a, b):
    return jnp.dot(a, b, preferred_element_type=f32)


def dot_t(a, b):
    return lax.dot_general(a, b, (((1,), (1,)), ((), ())), preferred_element_type=f32)


def lanes(index, size):
    return pl.ds(pl.multiple_of(index * size, size), size)


def remote(src, dst, send, recv, device):
    return pltpu.make_async_remote_copy(
        src_ref=src, dst_ref=dst, send_sem=send, recv_sem=recv,
        device_id=(device,), device_id_type=MESH,
    )


def read(ref, lead, m):
    pieces = [ref[*lead, :, 2 * m + i].reshape(GRID, 128) for i in range(2)]
    return jnp.concatenate(pieces, axis=1)


def kernel(
    orb, kv, shell, left, four, forward, backward, exch, margin,
    fields, work, total, screen, classes, w_high, w_low, v_high, v_low,
    grid_orb, grid_term, gram, rows,
    load_sem, send_sem, recv_sem, many_send, many_recv, out_sem,
):
    me = lax.axis_index("band")
    core = lax.rem(me, 2)
    x = lax.rem(me // 2, 4)
    plane = me // 8
    partner = me + 1 - 2 * core
    first = lax.rem(me + BANDS - 2 + 4 * core, BANDS)
    second = lax.rem(me + 2 - 4 * core + BANDS, BANDS)

    def wrap4(v):
        return lax.rem(v + 4, 4)

    load = pltpu.make_async_copy(orb, fields.at[0], load_sem.at[0])
    load.start()
    load_classes = pltpu.make_async_copy(shell, classes, load_sem.at[1])
    load_classes.start()
    load.wait()

    to_first = remote(fields.at[0], fields.at[2], send_sem.at[0], recv_sem.at[2], first)
    to_partner = remote(fields.at[0], fields.at[1], send_sem.at[1], recv_sem.at[1], partner)
    to_second = remote(fields.at[0], fields.at[4], send_sem.at[2], recv_sem.at[4], second)
    forward_on = remote(fields.at[2], fields.at[3], send_sem.at[3], recv_sem.at[3], partner)
    to_first.start()
    to_partner.start()

    def send_slice(slot, orbital, owner):
        remote(
            fields.at[slot, lax.rem(owner, 8), pl.ds(owner // 8 * 2, 2)],
            grid_orb.at[pl.ds(orbital * 2, 2)],
            many_send.at[0], many_recv.at[0], owner,
        ).start()

    def send_near(slot, orbital):
        def one(t, carry):
            there = lax.rem(plane + t // 2, 16)
            side = lax.rem(core + t, 2)
            send_slice(slot, orbital, there * 8 + x * 2 + side)
            return carry

        lax.fori_loop(1, 32, one, 0)
        grid_orb[pl.ds(orbital * 2, 2)] = fields[slot, lax.rem(me, 8), pl.ds(plane * 2, 2)]

    def send_across(slot, orbital, x_there, side):
        def one(t, carry):
            there = lax.rem(plane + t, 16)
            send_slice(slot, orbital, there * 8 + x_there * 2 + side)
            return carry

        lax.fori_loop(0, 16, one, 0)

    send_near(0, me)

    def make_tables(k, carry):
        for q in range(4):
            rows_here = pl.ds(q * GRID, GRID)
            high, low = split(four[...] * forward[pl.ds(k * 4 + q, 1), :])
            w_high[k, rows_here, :] = high
            w_low[k, rows_here, :] = low
            high, low = split(four[...] * backward[pl.ds(k * 4 + q, 1), :])
            v_high[k, rows_here, :] = high
            v_low[k, rows_here, :] = low
        return carry

    lax.fori_loop(0, TILES, make_tables, 0)

    load_classes.wait()
    values = [kv[i] * (-1.0 / GRID**3) for i in range(32)]

    def look_up(index):
        level = values
        bit = 1
        while len(level) > 1:
            picked = (index & bit) != 0
            level = [
                jnp.where(picked, level[i + 1], level[i]) for i in range(0, len(level), 2)
            ]
            bit *= 2
        return level[0]

    def make_screen(g, carry):
        here = lanes(g, 8)
        left_half = lax.broadcasted_iota(jnp.int32, (8, 128), 1) < GRID

        def chunk(i):
            return classes[here, pl.ds(i * 128, 128)]

        def turned(i):
            return pltpu.roll(chunk(i), GRID, 1)

        for k in range(TILES):
            if k == 0:
                pair = (
                    jnp.where(left_half, chunk(0), turned(16)),
                    jnp.where(left_half, chunk(8), turned(24)),
                )
                screen[here, pl.ds(0, 128)] = look_up(pair[0])
                screen[here, pl.ds(128, 128)] = look_up(pair[1])
                continue
            if k % 2 == 0:
                mixed = jnp.where(left_half, chunk(k // 2), turned((32 - k) // 2))
            else:
                mixed = jnp.where(left_half, turned((k - 1) // 2), chunk((31 - k) // 2))
            found = look_up(mixed)
            screen[here, pl.ds(k * 256, 128)] = found
            screen[here, pl.ds(k * 256 + 128, 128)] = found
        return carry

    lax.fori_loop(0, 8, make_screen, 0)
    total[...] = jnp.zeros_like(total)

    def left_pass(value):
        high, low = split(value)
        return dot(left[...], jnp.concatenate([high, high, low], axis=0))

    def send_terms(j):
        def one(g, carry):
            owner = j * 8 + g

            @pl.when(owner != me)
            def _():
                remote(
                    total.at[g, pl.ds(j * 2, 2)],
                    grid_term.at[pl.ds(me * 2, 2)],
                    many_send.at[1], many_recv.at[1], owner,
                ).start()

            return carry

        lax.fori_loop(0, 8, one, 0)

    def one_pair(it, carry):
        @pl.when(it == 1)
        def _():
            to_partner.wait_recv()

        @pl.when(it == 2)
        def _():
            to_first.wait_send()
            to_second.start()
            to_first.wait_recv()
            forward_on.start()
            send_near(2, second)
            send_across(2, second, wrap4(x - 1 + 2 * core), 1 - core)

        @pl.when(it == 3)
        def _():
            forward_on.wait_recv()

        @pl.when(it == 4)
        def _():
            to_second.wait_recv()
            send_near(4, first)
            send_across(4, first, wrap4(x + 1 - 2 * core), core)

        def first_stage(m, c):
            here = lanes(m, 256)
            work[:, here] = left_pass(read(fields, (0,), m) * read(fields, (it,), m))
            return c

        lax.fori_loop(0, 16, first_stage, 0)

        def second_stage(g, c):
            here = lanes(g, 8)
            re, im = half_spectrum([work[here, pl.ds(n * 128, 128)] for n in range(32)])
            work[here, pl.ds(0, 128)] = re[0]
            work[here, pl.ds(128, 128)] = re[16]
            for k in range(1, 16):
                work[here, pl.ds(k * 256, 128)] = re[k]
                work[here, pl.ds(k * 256 + 128, 128)] = im[k]
            return c

        lax.fori_loop(0, 8, second_stage, 0)

        def third_stage(k, c):
            here = lanes(k, 256)
            high, low = split(work[:, here])
            spectrum = dot(high, w_high[k]) + dot(low, w_high[k]) + dot(high, w_low[k])
            high, low = split(spectrum * screen[:, here])
            work[:, here] = dot(high, v_high[k]) + dot(low, v_high[k]) + dot(high, v_low[k])
            return c

        lax.fori_loop(0, 16, third_stage, 0)

        def fourth_stage(g, c):
            here = lanes(g, 8)
            re = [work[here, pl.ds(0, 128)]]
            im = [None]
            for k in range(1, 16):
                re.append(work[here, pl.ds(k * 256, 128)])
                im.append(work[here, pl.ds(k * 256 + 128, 128)])
            re.append(work[here, pl.ds(128, 128)])
            im.append(None)
            out = half_spectrum_transposed(re, im)
            for n in range(32):
                work[here, pl.ds(n * 128, 128)] = out[n]
            return c

        lax.fori_loop(0, 8, fourth_stage, 0)

        def fifth_stage(m, c):
            j = lax.rem(plane + m, 16)
            added = left_pass(work[:, lanes(j, 256)])
            for i in range(2):
                part = added[:, i * 128 : i * 128 + 128].reshape(8, 8, 128)
                total[:, 2 * j + i] += part * fields[it, :, 2 * j + i]

            @pl.when(jnp.logical_and(it == 4, m > 0))
            def _():
                send_terms(lax.rem(plane + m + 15, 16))

            return c

        lax.fori_loop(0, 16, fifth_stage, 0)
        return carry

    lax.fori_loop(0, 5, one_pair, 0)
    send_terms(lax.rem(plane + 15, 16))
    write = pltpu.make_async_copy(total, exch, out_sem)
    write.start()
    grid_term[pl.ds(me * 2, 2)] = total[lax.rem(me, 8), pl.ds(plane * 2, 2)]

    def wait_many(count, buffer, index):
        part = buffer.at[pl.ds(0, count)]
        remote(part, part, many_send.at[index], many_recv.at[index], partner).wait_recv()

    wait_many(125 * 2, grid_orb, 0)
    wait_many(127 * 2, grid_term, 1)
    def across(buffer, s):
        flat = buffer.reshape(BANDS * 16, 128)
        return jnp.concatenate(
            [flat[pl.ds(8 * i + s, BANDS, stride=16), :] for i in range(2)], axis=1
        )

    result = jnp.zeros((BANDS, BANDS), f32)
    for s in range(8):
        a_high, a_low = split(across(grid_orb, s))
        b_high, b_low = split(across(grid_term, s))
        result += dot_t(a_high, b_high) + dot_t(a_low, b_high) + dot_t(a_high, b_low)
    result = result * (1.0 / GRID**3)
    for i in range(BANDS):
        gram[i] = result[i : i + 1, :]

    def send_row(t, carry):
        owner = lax.rem(me + t, BANDS)
        remote(
            gram.at[owner], rows.at[me], many_send.at[2], many_recv.at[2], owner
        ).start()
        return carry

    lax.fori_loop(1, BANDS, send_row, 0)
    rows[me] = gram[me]
    part = rows.at[pl.ds(0, BANDS - 1)]
    remote(part, part, many_send.at[2], many_recv.at[2], partner).wait_recv()
    margin[...] = jnp.sum(rows[...], axis=0)

    to_partner.wait_send()
    to_second.wait_send()
    forward_on.wait_send()
    part = grid_orb.at[pl.ds(0, 125 * 2)]
    remote(part, part, many_send.at[0], many_recv.at[0], partner).wait_send()
    part = grid_term.at[pl.ds(0, 127 * 2)]
    remote(part, part, many_send.at[1], many_recv.at[1], partner).wait_send()
    part = rows.at[pl.ds(0, BANDS - 1)]
    remote(part, part, many_send.at[2], many_recv.at[2], partner).wait_send()
    write.wait()


def local(orbitals, kernel_values, shell_index):
    any_space = pl.BlockSpec(memory_space=pl.ANY)
    vmem = pl.BlockSpec(memory_space=pltpu.VMEM)
    exchange, margin = pl.pallas_call(
        kernel,
        out_shape=(
            jax.ShapeDtypeStruct(TILED, f32),
            jax.ShapeDtypeStruct((1, BANDS), f32),
        ),
        in_specs=[any_space, pl.BlockSpec(memory_space=pltpu.SMEM), any_space] + [vmem] * 4,
        out_specs=(any_space, vmem),
        scratch_shapes=[
            pltpu.VMEM((5, *TILED), f32),
            pltpu.VMEM((GRID, WIDE), f32),
            pltpu.VMEM(TILED, f32),
            pltpu.VMEM((GRID, WIDE), f32),
            pltpu.VMEM((GRID, WIDE), jnp.int32),
            pltpu.VMEM((TILES, 256, 256), bf16),
            pltpu.VMEM((TILES, 256, 256), bf16),
            pltpu.VMEM((TILES, 256, 256), bf16),
            pltpu.VMEM((TILES, 256, 256), bf16),
            pltpu.VMEM((BANDS * 2, 8, 128), f32),
            pltpu.VMEM((BANDS * 2, 8, 128), f32),
            pltpu.VMEM((BANDS, 1, BANDS), f32),
            pltpu.VMEM((BANDS, 1, BANDS), f32),
            pltpu.SemaphoreType.DMA((2,)),
            pltpu.SemaphoreType.DMA((4,)),
            pltpu.SemaphoreType.DMA((5,)),
            pltpu.SemaphoreType.DMA((3,)),
            pltpu.SemaphoreType.DMA((3,)),
            pltpu.SemaphoreType.DMA,
        ],
        compiler_params=pltpu.CompilerParams(
            has_side_effects=True, vmem_limit_bytes=56 * 1024 * 1024
        ),
        name="exchange",
    )(
        orbitals.reshape(8, 8, 32, 128).transpose(0, 2, 1, 3),
        kernel_values,
        shell_index,
        *[jnp.asarray(c) for c in constants()],
    )
    return exchange.transpose(0, 2, 1, 3).reshape(1, GRID, WIDE), margin


def solution(mesh):
    return jax.shard_map(
        local,
        mesh=mesh,
        in_specs=(P("band", None, None), P(), P()),
        out_specs=(P("band", None, None), P("band", None)),
        check_vma=False,
    )
```

```python
import math

import jax
import jax.numpy as jnp
import numpy as np
from jax import lax
from jax.experimental import pallas as pl
from jax.experimental.pallas import tpu as pltpu
from jax.sharding import PartitionSpec as P

GRID = 64
WIDE = GRID * GRID
BANDS = 128
TILES = 16
TILED = (8, 32, 8, 128)
MESH = pl.DeviceIdType.MESH
f32 = jnp.float32
bf16 = jnp.bfloat16


def cas(angle):
    return math.cos(angle) + math.sin(angle)


def cas_table():
    index = np.arange(GRID)
    angle = 2.0 * math.pi / GRID * (index[:, None] * index[None] % GRID)
    return np.cos(angle) + np.sin(angle)


def frequencies(k):
    return (0, 32, 16, 48) if k == 0 else (k, 32 - k, 64 - k, 32 + k)


def mixing(k):
    table = np.zeros((4, 4))
    for t, b in enumerate(frequencies(k)):
        for q in range(4):
            part, r = q // 2, q % 2
            angle = 2.0 * math.pi * b * r / GRID
            if k == 0:
                table[q, t] = cas(angle) if (part == 0) == (b % 32 == 0) else 0.0
            elif part == 0:
                table[q, t] = cas(angle)
            else:
                sign = 1.0 if b in (k, 32 + k) else -1.0
                table[q, t] = sign * (math.sin(angle) - math.cos(angle))
    return table


def constants():
    table = cas_table()
    high = table.astype(np.float32).astype(bf16)
    low = (table - high.astype(np.float64)).astype(np.float32).astype(bf16)
    left = np.concatenate([high, low, high], axis=1)
    four = np.tile(table, (1, 4)).astype(np.float32)
    mixes = np.stack([mixing(k) for k in range(TILES)])
    forward = np.repeat(mixes.reshape(TILES * 4, 4), GRID, axis=1).astype(np.float32)
    backward = np.repeat(
        np.swapaxes(mixes, 1, 2).reshape(TILES * 4, 4), GRID, axis=1
    ).astype(np.float32)
    return left, four, forward, backward


def half_spectrum(xs):
    n = len(xs)
    if n == 2:
        return [xs[0] + xs[1], xs[0] - xs[1]], [None, None]
    even_re, even_im = half_spectrum(xs[0::2])
    odd_re, odd_im = half_spectrum(xs[1::2])
    h, q = n // 2, n // 4
    re, im = [None] * (h + 1), [None] * (h + 1)
    re[0], re[h] = even_re[0] + odd_re[0], even_re[0] - odd_re[0]
    for k in range(1, q):
        c, s = math.cos(2 * math.pi * k / n), -math.sin(2 * math.pi * k / n)
        if 2 * k == q:
            t_re, t_im = (odd_re[k] + odd_im[k]) * c, (odd_im[k] - odd_re[k]) * c
        else:
            t_re = odd_re[k] * c - odd_im[k] * s
            t_im = odd_re[k] * s + odd_im[k] * c
        re[k], im[k] = even_re[k] + t_re, even_im[k] + t_im
        re[h - k], im[h - k] = even_re[k] - t_re, t_im - even_im[k]
    re[q], im[q] = even_re[q], -odd_re[q]
    return re, im


def half_spectrum_transposed(re, im):
    h = len(re) - 1
    n = 2 * h
    if n == 2:
        return [re[0] + re[1], re[0] - re[1]]
    q = n // 4
    even_re, even_im = [None] * (q + 1), [None] * (q + 1)
    odd_re, odd_im = [None] * (q + 1), [None] * (q + 1)
    even_re[0], odd_re[0] = re[0] + re[h], re[0] - re[h]
    for k in range(1, q):
        even_re[k], even_im[k] = re[k] + re[h - k], im[k] - im[h - k]
        d_re, d_im = re[k] - re[h - k], im[k] + im[h - k]
        c, s = math.cos(2 * math.pi * k / n), math.sin(2 * math.pi * k / n)
        if 2 * k == q:
            odd_re[k], odd_im[k] = (d_re - d_im) * c, (d_re + d_im) * c
        else:
            odd_re[k], odd_im[k] = d_re * c - d_im * s, d_re * s + d_im * c
    even_re[q], odd_re[q] = re[q], -im[q]
    out = [None] * n
    out[0::2] = half_spectrum_transposed(even_re, even_im)
    out[1::2] = half_spectrum_transposed(odd_re, odd_im)
    return out


def split(x):
    high = x.astype(bf16)
    return high, (x - high.astype(f32)).astype(bf16)


def dot(a, b):
    return jnp.dot(a, b, preferred_element_type=f32)


def dot_t(a, b):
    return lax.dot_general(a, b, (((1,), (1,)), ((), ())), preferred_element_type=f32)


def lanes(index, size):
    return pl.ds(pl.multiple_of(index * size, size), size)


def remote(src, dst, send, recv, device):
    return pltpu.make_async_remote_copy(
        src_ref=src, dst_ref=dst, send_sem=send, recv_sem=recv,
        device_id=(device,), device_id_type=MESH,
    )


def read(ref, lead, m):
    pieces = [ref[*lead, :, 2 * m + i].reshape(GRID, 128) for i in range(2)]
    return jnp.concatenate(pieces, axis=1)


def kernel(
    orb, kv, shell, left, four, forward, backward, exch, margin,
    fields, work, total, screen, classes, w_high, w_low, v_high, v_low,
    grid_orb, grid_term, gram, rows,
    load_sem, send_sem, recv_sem, many_send, many_recv, out_sem,
):
    me = lax.axis_index("band")
    core = lax.rem(me, 2)
    x = lax.rem(me // 2, 4)
    plane = me // 8
    partner = me + 1 - 2 * core
    first = lax.rem(me + BANDS - 2 + 4 * core, BANDS)
    second = lax.rem(me + 2 - 4 * core + BANDS, BANDS)

    def wrap4(v):
        return lax.rem(v + 4, 4)

    load = pltpu.make_async_copy(orb, fields.at[0], load_sem.at[0])
    load.start()
    load_classes = pltpu.make_async_copy(shell, classes, load_sem.at[1])
    load_classes.start()
    load.wait()

    to_first = remote(fields.at[0], fields.at[2], send_sem.at[0], recv_sem.at[2], first)
    to_partner = remote(fields.at[0], fields.at[1], send_sem.at[1], recv_sem.at[1], partner)
    to_second = remote(fields.at[0], fields.at[4], send_sem.at[2], recv_sem.at[4], second)
    forward_on = remote(fields.at[2], fields.at[3], send_sem.at[3], recv_sem.at[3], partner)
    to_first.start()
    to_partner.start()

    def send_slice(slot, orbital, owner):
        remote(
            fields.at[slot, lax.rem(owner, 8), pl.ds(owner // 8 * 2, 2)],
            grid_orb.at[pl.ds(orbital * 2, 2)],
            many_send.at[0], many_recv.at[0], owner,
        ).start()

    def send_near(slot, orbital):
        def one(t, carry):
            there = lax.rem(plane + t // 2, 16)
            side = lax.rem(core + t, 2)
            send_slice(slot, orbital, there * 8 + x * 2 + side)
            return carry

        lax.fori_loop(1, 32, one, 0)
        grid_orb[pl.ds(orbital * 2, 2)] = fields[slot, lax.rem(me, 8), pl.ds(plane * 2, 2)]

    def send_across(slot, orbital, x_there, side):
        def one(t, carry):
            there = lax.rem(plane + t, 16)
            send_slice(slot, orbital, there * 8 + x_there * 2 + side)
            return carry

        lax.fori_loop(0, 16, one, 0)

    send_near(0, me)

    def make_tables(k, carry):
        for q in range(4):
            rows_here = pl.ds(q * GRID, GRID)
            high, low = split(four[...] * forward[pl.ds(k * 4 + q, 1), :])
            w_high[k, rows_here, :] = high
            w_low[k, rows_here, :] = low
            high, low = split(four[...] * backward[pl.ds(k * 4 + q, 1), :])
            v_high[k, rows_here, :] = high
            v_low[k, rows_here, :] = low
        return carry

    lax.fori_loop(0, TILES, make_tables, 0)

    load_classes.wait()
    values = [kv[i] * (-1.0 / GRID**3) for i in range(32)]

    def look_up(index):
        level = values
        bit = 1
        while len(level) > 1:
            picked = (index & bit) != 0
            level = [
                jnp.where(picked, level[i + 1], level[i]) for i in range(0, len(level), 2)
            ]
            bit *= 2
        return level[0]

    def make_screen(g, carry):
        here = lanes(g, 8)
        left_half = lax.broadcasted_iota(jnp.int32, (8, 128), 1) < GRID

        def chunk(i):
            return classes[here, pl.ds(i * 128, 128)]

        def turned(i):
            return pltpu.roll(chunk(i), GRID, 1)

        for k in range(TILES):
            if k == 0:
                pair = (
                    jnp.where(left_half, chunk(0), turned(16)),
                    jnp.where(left_half, chunk(8), turned(24)),
                )
                screen[here, pl.ds(0, 128)] = look_up(pair[0])
                screen[here, pl.ds(128, 128)] = look_up(pair[1])
                continue
            if k % 2 == 0:
                mixed = jnp.where(left_half, chunk(k // 2), turned((32 - k) // 2))
            else:
                mixed = jnp.where(left_half, turned((k - 1) // 2), chunk((31 - k) // 2))
            found = look_up(mixed)
            screen[here, pl.ds(k * 256, 128)] = found
            screen[here, pl.ds(k * 256 + 128, 128)] = found
        return carry

    lax.fori_loop(0, 8, make_screen, 0)
    total[...] = jnp.zeros_like(total)

    def left_pass(value):
        high, low = split(value)
        return dot(left[...], jnp.concatenate([high, high, low], axis=0))

    def send_terms(j):
        def one(g, carry):
            owner = j * 8 + g

            @pl.when(owner != me)
            def _():
                remote(
                    total.at[g, pl.ds(j * 2, 2)],
                    grid_term.at[pl.ds(me * 2, 2)],
                    many_send.at[1], many_recv.at[1], owner,
                ).start()

            return carry

        lax.fori_loop(0, 8, one, 0)

    def one_pair(it, carry):
        @pl.when(it == 1)
        def _():
            to_partner.wait_recv()

        @pl.when(it == 2)
        def _():
            to_first.wait_send()
            to_second.start()
            to_first.wait_recv()
            forward_on.start()
            send_near(2, second)
            send_across(2, second, wrap4(x - 1 + 2 * core), 1 - core)

        @pl.when(it == 3)
        def _():
            forward_on.wait_recv()

        @pl.when(it == 4)
        def _():
            to_second.wait_recv()
            send_near(4, first)
            send_across(4, first, wrap4(x + 1 - 2 * core), core)

        def first_stage(m, c):
            here = lanes(m, 256)
            work[:, here] = left_pass(read(fields, (0,), m) * read(fields, (it,), m))
            return c

        lax.fori_loop(0, 16, first_stage, 0, unroll=True)

        def second_stage(g, c):
            here = lanes(g, 8)
            re, im = half_spectrum([work[here, pl.ds(n * 128, 128)] for n in range(32)])
            work[here, pl.ds(0, 128)] = re[0]
            work[here, pl.ds(128, 128)] = re[16]
            for k in range(1, 16):
                work[here, pl.ds(k * 256, 128)] = re[k]
                work[here, pl.ds(k * 256 + 128, 128)] = im[k]
            return c

        lax.fori_loop(0, 8, second_stage, 0)

        def third_stage(k, c):
            here = lanes(k, 256)
            high, low = split(work[:, here])
            spectrum = dot(high, w_high[k]) + dot(low, w_high[k]) + dot(high, w_low[k])
            high, low = split(spectrum * screen[:, here])
            work[:, here] = dot(high, v_high[k]) + dot(low, v_high[k]) + dot(high, v_low[k])
            return c

        lax.fori_loop(0, 16, third_stage, 0, unroll=True)

        def fourth_stage(g, c):
            here = lanes(g, 8)
            re = [work[here, pl.ds(0, 128)]]
            im = [None]
            for k in range(1, 16):
                re.append(work[here, pl.ds(k * 256, 128)])
                im.append(work[here, pl.ds(k * 256 + 128, 128)])
            re.append(work[here, pl.ds(128, 128)])
            im.append(None)
            out = half_spectrum_transposed(re, im)
            for n in range(32):
                work[here, pl.ds(n * 128, 128)] = out[n]
            return c

        lax.fori_loop(0, 8, fourth_stage, 0)

        def fifth_stage(m, c):
            j = lax.rem(plane + m, 16)
            added = left_pass(work[:, lanes(j, 256)])
            for i in range(2):
                part = added[:, i * 128 : i * 128 + 128].reshape(8, 8, 128)
                total[:, 2 * j + i] += part * fields[it, :, 2 * j + i]

            if m > 0:

                @pl.when(it == 4)
                def _():
                    send_terms(lax.rem(plane + m + 15, 16))

            return c

        for m in range(16):
            fifth_stage(m, 0)
        return carry

    lax.fori_loop(0, 5, one_pair, 0)
    send_terms(lax.rem(plane + 15, 16))
    write = pltpu.make_async_copy(total, exch, out_sem)
    write.start()
    grid_term[pl.ds(me * 2, 2)] = total[lax.rem(me, 8), pl.ds(plane * 2, 2)]

    def wait_many(count, buffer, index):
        part = buffer.at[pl.ds(0, count)]
        remote(part, part, many_send.at[index], many_recv.at[index], partner).wait_recv()

    wait_many(125 * 2, grid_orb, 0)
    wait_many(127 * 2, grid_term, 1)
    def across(buffer, s):
        flat = buffer.reshape(BANDS * 16, 128)
        return jnp.concatenate(
            [flat[pl.ds(8 * i + s, BANDS, stride=16), :] for i in range(2)], axis=1
        )

    result = jnp.zeros((BANDS, BANDS), f32)
    for s in range(8):
        a_high, a_low = split(across(grid_orb, s))
        b_high, b_low = split(across(grid_term, s))
        result += dot_t(a_high, b_high) + dot_t(a_low, b_high) + dot_t(a_high, b_low)
    result = result * (1.0 / GRID**3)
    for i in range(BANDS):
        gram[i] = result[i : i + 1, :]

    def send_row(t, carry):
        owner = lax.rem(me + t, BANDS)
        remote(
            gram.at[owner], rows.at[me], many_send.at[2], many_recv.at[2], owner
        ).start()
        return carry

    lax.fori_loop(1, BANDS, send_row, 0)
    rows[me] = gram[me]
    part = rows.at[pl.ds(0, BANDS - 1)]
    remote(part, part, many_send.at[2], many_recv.at[2], partner).wait_recv()
    margin[...] = jnp.sum(rows[...], axis=0)

    to_partner.wait_send()
    to_second.wait_send()
    forward_on.wait_send()
    part = grid_orb.at[pl.ds(0, 125 * 2)]
    remote(part, part, many_send.at[0], many_recv.at[0], partner).wait_send()
    part = grid_term.at[pl.ds(0, 127 * 2)]
    remote(part, part, many_send.at[1], many_recv.at[1], partner).wait_send()
    part = rows.at[pl.ds(0, BANDS - 1)]
    remote(part, part, many_send.at[2], many_recv.at[2], partner).wait_send()
    write.wait()


def local(orbitals, kernel_values, shell_index):
    any_space = pl.BlockSpec(memory_space=pl.ANY)
    vmem = pl.BlockSpec(memory_space=pltpu.VMEM)
    exchange, margin = pl.pallas_call(
        kernel,
        out_shape=(
            jax.ShapeDtypeStruct(TILED, f32),
            jax.ShapeDtypeStruct((1, BANDS), f32),
        ),
        in_specs=[any_space, pl.BlockSpec(memory_space=pltpu.SMEM), any_space] + [vmem] * 4,
        out_specs=(any_space, vmem),
        scratch_shapes=[
            pltpu.VMEM((5, *TILED), f32),
            pltpu.VMEM((GRID, WIDE), f32),
            pltpu.VMEM(TILED, f32),
            pltpu.VMEM((GRID, WIDE), f32),
            pltpu.VMEM((GRID, WIDE), jnp.int32),
            pltpu.VMEM((TILES, 256, 256), bf16),
            pltpu.VMEM((TILES, 256, 256), bf16),
            pltpu.VMEM((TILES, 256, 256), bf16),
            pltpu.VMEM((TILES, 256, 256), bf16),
            pltpu.VMEM((BANDS * 2, 8, 128), f32),
            pltpu.VMEM((BANDS * 2, 8, 128), f32),
            pltpu.VMEM((BANDS, 1, BANDS), f32),
            pltpu.VMEM((BANDS, 1, BANDS), f32),
            pltpu.SemaphoreType.DMA((2,)),
            pltpu.SemaphoreType.DMA((4,)),
            pltpu.SemaphoreType.DMA((5,)),
            pltpu.SemaphoreType.DMA((3,)),
            pltpu.SemaphoreType.DMA((3,)),
            pltpu.SemaphoreType.DMA,
        ],
        compiler_params=pltpu.CompilerParams(
            has_side_effects=True, vmem_limit_bytes=56 * 1024 * 1024
        ),
        name="exchange",
    )(
        orbitals.reshape(8, 8, 32, 128).transpose(0, 2, 1, 3),
        kernel_values,
        shell_index,
        *[jnp.asarray(c) for c in constants()],
    )
    return exchange.transpose(0, 2, 1, 3).reshape(1, GRID, WIDE), margin


def solution(mesh):
    return jax.shard_map(
        local,
        mesh=mesh,
        in_specs=(P("band", None, None), P(), P()),
        out_specs=(P("band", None, None), P("band", None)),
        check_vma=False,
    )
```

```python
import math

import jax
import jax.numpy as jnp
import numpy as np
from jax import lax
from jax.experimental import pallas as pl
from jax.experimental.pallas import tpu as pltpu
from jax.sharding import PartitionSpec as P

GRID = 64
WIDE = GRID * GRID
BANDS = 128
TILES = 16
TILED = (8, 32, 8, 128)
SHIFTS = sorted(
    ((dz, dy) for dz in range(4) for dy in range(4)),
    key=lambda s: -min(s[0], 4 - s[0]) - min(s[1], 4 - s[1]),
)
MESH = pl.DeviceIdType.MESH
f32 = jnp.float32
bf16 = jnp.bfloat16


def cas(angle):
    return math.cos(angle) + math.sin(angle)


def cas_table():
    index = np.arange(GRID)
    angle = 2.0 * math.pi / GRID * (index[:, None] * index[None] % GRID)
    return np.cos(angle) + np.sin(angle)


def frequencies(k):
    return (0, 32, 16, 48) if k == 0 else (k, 32 - k, 64 - k, 32 + k)


def mixing(k):
    table = np.zeros((4, 4))
    for t, b in enumerate(frequencies(k)):
        for q in range(4):
            part, r = q // 2, q % 2
            angle = 2.0 * math.pi * b * r / GRID
            if k == 0:
                table[q, t] = cas(angle) if (part == 0) == (b % 32 == 0) else 0.0
            elif part == 0:
                table[q, t] = cas(angle)
            else:
                sign = 1.0 if b in (k, 32 + k) else -1.0
                table[q, t] = sign * (math.sin(angle) - math.cos(angle))
    return table


def constants():
    table = cas_table()
    high = table.astype(np.float32).astype(bf16)
    low = (table - high.astype(np.float64)).astype(np.float32).astype(bf16)
    left = np.concatenate([high, low, high], axis=1)
    four = np.tile(table, (1, 4)).astype(np.float32)
    mixes = np.stack([mixing(k) for k in range(TILES)])
    forward = np.repeat(mixes.reshape(TILES * 4, 4), GRID, axis=1).astype(np.float32)
    backward = np.repeat(
        np.swapaxes(mixes, 1, 2).reshape(TILES * 4, 4), GRID, axis=1
    ).astype(np.float32)
    return left, four, forward, backward


def half_spectrum(xs):
    n = len(xs)
    if n == 2:
        return [xs[0] + xs[1], xs[0] - xs[1]], [None, None]
    even_re, even_im = half_spectrum(xs[0::2])
    odd_re, odd_im = half_spectrum(xs[1::2])
    h, q = n // 2, n // 4
    re, im = [None] * (h + 1), [None] * (h + 1)
    re[0], re[h] = even_re[0] + odd_re[0], even_re[0] - odd_re[0]
    for k in range(1, q):
        c, s = math.cos(2 * math.pi * k / n), -math.sin(2 * math.pi * k / n)
        if 2 * k == q:
            t_re, t_im = (odd_re[k] + odd_im[k]) * c, (odd_im[k] - odd_re[k]) * c
        else:
            t_re = odd_re[k] * c - odd_im[k] * s
            t_im = odd_re[k] * s + odd_im[k] * c
        re[k], im[k] = even_re[k] + t_re, even_im[k] + t_im
        re[h - k], im[h - k] = even_re[k] - t_re, t_im - even_im[k]
    re[q], im[q] = even_re[q], -odd_re[q]
    return re, im


def half_spectrum_transposed(re, im):
    h = len(re) - 1
    n = 2 * h
    if n == 2:
        return [re[0] + re[1], re[0] - re[1]]
    q = n // 4
    even_re, even_im = [None] * (q + 1), [None] * (q + 1)
    odd_re, odd_im = [None] * (q + 1), [None] * (q + 1)
    even_re[0], odd_re[0] = re[0] + re[h], re[0] - re[h]
    for k in range(1, q):
        even_re[k], even_im[k] = re[k] + re[h - k], im[k] - im[h - k]
        d_re, d_im = re[k] - re[h - k], im[k] + im[h - k]
        c, s = math.cos(2 * math.pi * k / n), math.sin(2 * math.pi * k / n)
        if 2 * k == q:
            odd_re[k], odd_im[k] = (d_re - d_im) * c, (d_re + d_im) * c
        else:
            odd_re[k], odd_im[k] = d_re * c - d_im * s, d_re * s + d_im * c
    even_re[q], odd_re[q] = re[q], -im[q]
    out = [None] * n
    out[0::2] = half_spectrum_transposed(even_re, even_im)
    out[1::2] = half_spectrum_transposed(odd_re, odd_im)
    return out


def split(x):
    high = x.astype(bf16)
    return high, (x - high.astype(f32)).astype(bf16)


def dot(a, b):
    return jnp.dot(a, b, preferred_element_type=f32)


def dot_t(a, b):
    return lax.dot_general(a, b, (((1,), (1,)), ((), ())), preferred_element_type=f32)


def lanes(index, size):
    return pl.ds(pl.multiple_of(index * size, size), size)


def remote(src, dst, send, recv, device):
    return pltpu.make_async_remote_copy(
        src_ref=src, dst_ref=dst, send_sem=send, recv_sem=recv,
        device_id=(device,), device_id_type=MESH,
    )


def read(ref, lead, m):
    pieces = [ref[*lead, :, 2 * m + i].reshape(GRID, 128) for i in range(2)]
    return jnp.concatenate(pieces, axis=1)


def kernel(
    orb, kv, shell, left_in, four_in, forward_in, backward_in, total, margin,
    fields, work, screen, classes, left, four, forward, backward,
    w_high, w_low, v_high, v_low, grid_orb, grid_term, gram, rows,
    load_sem, send_sem, recv_sem, part_send, part_recv, many_send, many_recv, meet_sem,
):
    me = lax.axis_index("band")
    core = lax.rem(me, 2)
    x = lax.rem(me // 2, 4)
    plane = me // 8
    partner = me + 1 - 2 * core
    first = lax.rem(me + BANDS - 2 + 4 * core, BANDS)
    second = lax.rem(me + 2 - 4 * core + BANDS, BANDS)

    def wrap4(v):
        return lax.rem(v + 4, 4)

    def plane_at(dz, dy):
        return wrap4(plane // 4 + dz) * 4 + wrap4(plane + dy)

    load = pltpu.make_async_copy(orb, fields.at[0], load_sem.at[0])
    load.start()

    meetings = [partner]
    neighbours = [first, second]
    for scale in (2, 8, 32):
        here = lax.rem(me // scale, 4)
        base = me - here * scale
        meetings.append(me + scale * (1 - 2 * lax.rem(here, 2)))
        meetings.append(base + scale * (3 - here))
    barrier = pltpu.get_barrier_semaphore()
    for device in neighbours + meetings:
        pl.semaphore_signal(barrier, inc=1, device_id=(device,), device_id_type=MESH)
    small = [
        pltpu.make_async_copy(src, dst, load_sem.at[i + 1])
        for i, (src, dst) in enumerate(
            [(four_in, four), (forward_in, forward), (backward_in, backward),
             (left_in, left), (shell, classes)]
        )
    ]
    for copy in small:
        copy.start()
    pl.semaphore_wait(barrier, len(neighbours + meetings))
    load.wait()

    to_partner = remote(fields.at[0], fields.at[1], send_sem.at[0], recv_sem.at[0], partner)
    forward_on = remote(fields.at[2], fields.at[3], send_sem.at[1], recv_sem.at[1], partner)

    def send_field(slot, part, device, below):
        start = 2 * lax.rem(device // 2, 4) - below + 8
        for i in range(8):
            group = lax.rem(start + i, 8)
            index = part if i < 3 else part + 1
            remote(
                fields.at[0, group], fields.at[slot, group],
                part_send.at[index], part_recv.at[index], device,
            ).start()

    def wait_field(slot, part):
        count = 3 if part % 2 == 0 else 5
        ref = fields.at[slot, pl.ds(0, count)]
        return remote(ref, ref, part_send.at[part], part_recv.at[part], partner)

    send_field(2, 0, first, 1 - core)
    to_partner.start()

    def send_slice(slot, orbital, owner):
        remote(
            fields.at[slot, lax.rem(owner, 8), pl.ds(owner // 8 * 2, 2)],
            grid_orb.at[pl.ds(orbital * 2, 2)],
            many_send.at[0], many_recv.at[0], owner,
        ).start()

    def send_near(slot, orbital):
        def one(t, carry):
            there = lax.rem(plane + t // 2, 16)
            side = lax.rem(core + t, 2)
            send_slice(slot, orbital, there * 8 + x * 2 + side)
            return carry

        lax.fori_loop(1, 32, one, 0)
        grid_orb[pl.ds(orbital * 2, 2)] = fields[slot, lax.rem(me, 8), pl.ds(plane * 2, 2)]

    def send_across(slot, orbital, x_there, side):
        def one(t, carry):
            there = lax.rem(plane + t, 16)
            send_slice(slot, orbital, there * 8 + x_there * 2 + side)
            return carry

        lax.fori_loop(0, 16, one, 0)

    def make_tables(k, carry):
        for q in range(4):
            rows_here = pl.ds(q * GRID, GRID)
            high, low = split(four[...] * forward[pl.ds(k * 4 + q, 1), :])
            w_high[k, rows_here, :] = high
            w_low[k, rows_here, :] = low
            high, low = split(four[...] * backward[pl.ds(k * 4 + q, 1), :])
            v_high[k, rows_here, :] = high
            v_low[k, rows_here, :] = low
        return carry

    for copy in small[:3]:
        copy.wait()
    for step, device in enumerate(meetings):
        pl.semaphore_signal(
            meet_sem.at[step], inc=1, device_id=(device,), device_id_type=MESH
        )
        lax.fori_loop(2 * step, 2 * step + 2, make_tables, 0)
        pl.semaphore_wait(meet_sem.at[step], 1)
    send_near(0, me)
    lax.fori_loop(14, TILES, make_tables, 0)

    for copy in small[3:]:
        copy.wait()
    values = [kv[i] * (-1.0 / GRID**3) for i in range(32)]

    def look_up(index):
        level = values
        bit = 1
        while len(level) > 1:
            picked = (index & bit) != 0
            level = [
                jnp.where(picked, level[i + 1], level[i]) for i in range(0, len(level), 2)
            ]
            bit *= 2
        return level[0]

    def make_screen(g, carry):
        here = lanes(g, 8)
        left_half = lax.broadcasted_iota(jnp.int32, (8, 128), 1) < GRID

        def chunk(i):
            return classes[here, pl.ds(i * 128, 128)]

        def turned(i):
            return pltpu.roll(chunk(i), GRID, 1)

        for k in range(TILES):
            if k == 0:
                pair = (
                    jnp.where(left_half, chunk(0), turned(16)),
                    jnp.where(left_half, chunk(8), turned(24)),
                )
                screen[here, pl.ds(0, 128)] = look_up(pair[0])
                screen[here, pl.ds(128, 128)] = look_up(pair[1])
                continue
            if k % 2 == 0:
                mixed = jnp.where(left_half, chunk(k // 2), turned((32 - k) // 2))
            else:
                mixed = jnp.where(left_half, turned((k - 1) // 2), chunk((31 - k) // 2))
            found = look_up(mixed)
            screen[here, pl.ds(k * 256, 128)] = found
            screen[here, pl.ds(k * 256 + 128, 128)] = found
        return carry

    lax.fori_loop(0, 8, make_screen, 0)
    total[...] = jnp.zeros_like(total)

    def left_pass(value):
        high, low = split(value)
        return dot(left[...], jnp.concatenate([high, high, low], axis=0))

    def send_terms(j):
        def one(g, carry):
            owner = j * 8 + g

            @pl.when(owner != me)
            def _():
                remote(
                    total.at[g, pl.ds(j * 2, 2)],
                    grid_term.at[pl.ds(me * 2, 2)],
                    many_send.at[1], many_recv.at[1], owner,
                ).start()

            return carry

        lax.fori_loop(0, 8, one, 0)

    def one_pair(it, carry):
        @pl.when(it == 1)
        def _():
            to_partner.wait_recv()

        @pl.when(it == 2)
        def _():
            for part in range(2):
                wait_field(2, part).wait_send()
            send_field(4, 2, second, core)
            wait_field(2, 0).wait_recv()
            send_near(2, second)
            send_across(2, second, wrap4(x - 1 + 2 * core), 1 - core)
            wait_field(2, 1).wait_recv()
            forward_on.start()

        @pl.when(it == 3)
        def _():
            forward_on.wait_recv()

        @pl.when(it == 4)
        def _():
            wait_field(4, 2).wait_recv()
            send_near(4, first)
            send_across(4, first, wrap4(x + 1 - 2 * core), core)
            wait_field(4, 3).wait_recv()

        def first_stage(m, c):
            here = lanes(m, 256)
            work[:, here] = left_pass(read(fields, (0,), m) * read(fields, (it,), m))
            return c

        lax.fori_loop(0, 16, first_stage, 0, unroll=True)

        def second_stage(g, c):
            here = lanes(g, 8)
            re, im = half_spectrum([work[here, pl.ds(n * 128, 128)] for n in range(32)])
            work[here, pl.ds(0, 128)] = re[0]
            work[here, pl.ds(128, 128)] = re[16]
            for k in range(1, 16):
                work[here, pl.ds(k * 256, 128)] = re[k]
                work[here, pl.ds(k * 256 + 128, 128)] = im[k]
            return c

        lax.fori_loop(0, 8, second_stage, 0)

        def third_stage(k, c):
            here = lanes(k, 256)
            high, low = split(work[:, here])
            spectrum = dot(high, w_high[k]) + dot(low, w_high[k]) + dot(high, w_low[k])
            high, low = split(spectrum * screen[:, here])
            work[:, here] = dot(high, v_high[k]) + dot(low, v_high[k]) + dot(high, v_low[k])
            return c

        lax.fori_loop(0, 16, third_stage, 0, unroll=True)

        def fourth_stage(g, c):
            here = lanes(g, 8)
            re = [work[here, pl.ds(0, 128)]]
            im = [None]
            for k in range(1, 16):
                re.append(work[here, pl.ds(k * 256, 128)])
                im.append(work[here, pl.ds(k * 256 + 128, 128)])
            re.append(work[here, pl.ds(128, 128)])
            im.append(None)
            out = half_spectrum_transposed(re, im)
            for n in range(32):
                work[here, pl.ds(n * 128, 128)] = out[n]
            return c

        lax.fori_loop(0, 8, fourth_stage, 0)

        for m, (dz, dy) in enumerate(SHIFTS):
            j = plane_at(dz, dy)
            added = left_pass(work[:, lanes(j, 256)])
            for i in range(2):
                part = added[:, i * 128 : i * 128 + 128].reshape(8, 8, 128)
                total[:, 2 * j + i] += part * fields[it, :, 2 * j + i]
            if m > 0:

                @pl.when(it == 4)
                def _():
                    send_terms(plane_at(*SHIFTS[m - 1]))

        return carry

    lax.fori_loop(0, 5, one_pair, 0)
    send_terms(plane)
    grid_term[pl.ds(me * 2, 2)] = total[lax.rem(me, 8), pl.ds(plane * 2, 2)]

    def wait_many(count, buffer, index):
        part = buffer.at[pl.ds(0, count)]
        remote(part, part, many_send.at[index], many_recv.at[index], partner).wait_recv()

    wait_many(125 * 2, grid_orb, 0)
    wait_many(127 * 2, grid_term, 1)
    def across(buffer, s):
        flat = buffer.reshape(BANDS * 16, 128)
        return jnp.concatenate(
            [flat[pl.ds(8 * i + s, BANDS, stride=16), :] for i in range(2)], axis=1
        )

    result = jnp.zeros((BANDS, BANDS), f32)
    for s in range(8):
        a_high, a_low = split(across(grid_orb, s))
        b_high, b_low = split(across(grid_term, s))
        result += dot_t(a_high, b_high) + dot_t(a_low, b_high) + dot_t(a_high, b_low)
    result = result * (1.0 / GRID**3)
    for i in range(BANDS):
        gram[i] = result[i : i + 1, :]

    def send_row(t, carry):
        owner = lax.rem(me + t, BANDS)
        remote(
            gram.at[owner], rows.at[me], many_send.at[2], many_recv.at[2], owner
        ).start()
        return carry

    lax.fori_loop(1, BANDS, send_row, 0)
    rows[me] = gram[me]
    part = rows.at[pl.ds(0, BANDS - 1)]
    remote(part, part, many_send.at[2], many_recv.at[2], partner).wait_recv()
    margin[...] = jnp.sum(rows[...], axis=0)

    to_partner.wait_send()
    forward_on.wait_send()
    for part in range(2, 4):
        wait_field(4, part).wait_send()
    part = grid_orb.at[pl.ds(0, 125 * 2)]
    remote(part, part, many_send.at[0], many_recv.at[0], partner).wait_send()
    part = grid_term.at[pl.ds(0, 127 * 2)]
    remote(part, part, many_send.at[1], many_recv.at[1], partner).wait_send()
    part = rows.at[pl.ds(0, BANDS - 1)]
    remote(part, part, many_send.at[2], many_recv.at[2], partner).wait_send()


def finish(total, margin, exch, out, sem):
    copy = pltpu.make_async_copy(total, exch, sem)
    copy.start()
    out[...] = margin[...]
    copy.wait()


def local(orbitals, kernel_values, shell_index):
    any_space = pl.BlockSpec(memory_space=pl.ANY)
    hbm = pl.BlockSpec(memory_space=pltpu.HBM)
    vmem = pl.BlockSpec(memory_space=pltpu.VMEM)
    tables = constants()
    total, margin = pl.pallas_call(
        kernel,
        out_shape=(pltpu.VMEM(TILED, f32), pltpu.VMEM((1, BANDS), f32)),
        in_specs=[hbm, pl.BlockSpec(memory_space=pltpu.SMEM)] + [hbm] * 5,
        out_specs=(vmem, vmem),
        scratch_shapes=[
            pltpu.VMEM((5, *TILED), f32),
            pltpu.VMEM((GRID, WIDE), f32),
            pltpu.VMEM((GRID, WIDE), f32),
            pltpu.VMEM((GRID, WIDE), jnp.int32),
            *[pltpu.VMEM(t.shape, t.dtype) for t in tables],
            *[pltpu.VMEM((TILES, 256, 256), bf16)] * 4,
            pltpu.VMEM((BANDS * 2, 8, 128), f32),
            pltpu.VMEM((BANDS * 2, 8, 128), f32),
            pltpu.VMEM((BANDS, 1, BANDS), f32),
            pltpu.VMEM((BANDS, 1, BANDS), f32),
            pltpu.SemaphoreType.DMA((6,)),
            pltpu.SemaphoreType.DMA((2,)),
            pltpu.SemaphoreType.DMA((2,)),
            pltpu.SemaphoreType.DMA((4,)),
            pltpu.SemaphoreType.DMA((4,)),
            pltpu.SemaphoreType.DMA((3,)),
            pltpu.SemaphoreType.DMA((3,)),
            pltpu.SemaphoreType.REGULAR((7,)),
        ],
        compiler_params=pltpu.CompilerParams(
            collective_id=0, has_side_effects=True, vmem_limit_bytes=62 * 1024 * 1024 + 768 * 1024
        ),
        name="exchange",
    )(
        orbitals.reshape(8, 8, 32, 128).transpose(0, 2, 1, 3),
        kernel_values,
        shell_index,
        *[jnp.asarray(c) for c in tables],
    )
    exchange, margin = pl.pallas_call(
        finish,
        out_shape=(
            jax.ShapeDtypeStruct(TILED, f32),
            jax.ShapeDtypeStruct((1, BANDS), f32),
        ),
        in_specs=[vmem, vmem],
        out_specs=(any_space, vmem),
        scratch_shapes=[pltpu.SemaphoreType.DMA],
        name="finish",
    )(
        pltpu.with_memory_space_constraint(total, pltpu.VMEM),
        pltpu.with_memory_space_constraint(margin, pltpu.VMEM),
    )
    return exchange.transpose(0, 2, 1, 3).reshape(1, GRID, WIDE), margin


def solution(mesh):
    return jax.shard_map(
        local,
        mesh=mesh,
        in_specs=(P("band", None, None), P(), P()),
        out_specs=(P("band", None, None), P("band", None)),
        check_vma=False,
    )
```

```python
import math

import jax
import jax.numpy as jnp
import numpy as np
from jax import lax
from jax.experimental import pallas as pl
from jax.experimental.pallas import tpu as pltpu
from jax.sharding import PartitionSpec as P

GRID = 64
WIDE = GRID * GRID
BANDS = 128
TILES = 16
SENT_TOGETHER = 4
RELAYED = 2
TILED = (8, 32, 8, 128)
SHIFTS = sorted(
    ((dz, dy) for dz in range(4) for dy in range(4)),
    key=lambda s: -min(s[0], 4 - s[0]) - min(s[1], 4 - s[1]),
)
MESH = pl.DeviceIdType.MESH
f32 = jnp.float32
bf16 = jnp.bfloat16


def cas(angle):
    return math.cos(angle) + math.sin(angle)


def cas_table():
    index = np.arange(GRID)
    angle = 2.0 * math.pi / GRID * (index[:, None] * index[None] % GRID)
    return np.cos(angle) + np.sin(angle)


def frequencies(k):
    return (0, 32, 16, 48) if k == 0 else (k, 32 - k, 64 - k, 32 + k)


def mixing(k):
    table = np.zeros((4, 4))
    for t, b in enumerate(frequencies(k)):
        for q in range(4):
            part, r = q // 2, q % 2
            angle = 2.0 * math.pi * b * r / GRID
            if k == 0:
                table[q, t] = cas(angle) if (part == 0) == (b % 32 == 0) else 0.0
            elif part == 0:
                table[q, t] = cas(angle)
            else:
                sign = 1.0 if b in (k, 32 + k) else -1.0
                table[q, t] = sign * (math.sin(angle) - math.cos(angle))
    return table


def constants():
    table = cas_table()
    high = table.astype(np.float32).astype(bf16)
    low = (table - high.astype(np.float64)).astype(np.float32).astype(bf16)
    left = np.concatenate([high, low, high], axis=1)
    four = np.tile(table, (1, 4)).astype(np.float32)
    mixes = np.stack([mixing(k) for k in range(TILES)])
    forward = np.repeat(mixes.reshape(TILES * 4, 4), GRID, axis=1).astype(np.float32)
    backward = np.repeat(
        np.swapaxes(mixes, 1, 2).reshape(TILES * 4, 4), GRID, axis=1
    ).astype(np.float32)
    return left, four, forward, backward


def half_spectrum(xs):
    n = len(xs)
    if n == 2:
        return [xs[0] + xs[1], xs[0] - xs[1]], [None, None]
    even_re, even_im = half_spectrum(xs[0::2])
    odd_re, odd_im = half_spectrum(xs[1::2])
    h, q = n // 2, n // 4
    re, im = [None] * (h + 1), [None] * (h + 1)
    re[0], re[h] = even_re[0] + odd_re[0], even_re[0] - odd_re[0]
    for k in range(1, q):
        c, s = math.cos(2 * math.pi * k / n), -math.sin(2 * math.pi * k / n)
        if 2 * k == q:
            t_re, t_im = (odd_re[k] + odd_im[k]) * c, (odd_im[k] - odd_re[k]) * c
        else:
            t_re = odd_re[k] * c - odd_im[k] * s
            t_im = odd_re[k] * s + odd_im[k] * c
        re[k], im[k] = even_re[k] + t_re, even_im[k] + t_im
        re[h - k], im[h - k] = even_re[k] - t_re, t_im - even_im[k]
    re[q], im[q] = even_re[q], -odd_re[q]
    return re, im


def half_spectrum_transposed(re, im):
    h = len(re) - 1
    n = 2 * h
    if n == 2:
        return [re[0] + re[1], re[0] - re[1]]
    q = n // 4
    even_re, even_im = [None] * (q + 1), [None] * (q + 1)
    odd_re, odd_im = [None] * (q + 1), [None] * (q + 1)
    even_re[0], odd_re[0] = re[0] + re[h], re[0] - re[h]
    for k in range(1, q):
        even_re[k], even_im[k] = re[k] + re[h - k], im[k] - im[h - k]
        d_re, d_im = re[k] - re[h - k], im[k] + im[h - k]
        c, s = math.cos(2 * math.pi * k / n), math.sin(2 * math.pi * k / n)
        if 2 * k == q:
            odd_re[k], odd_im[k] = (d_re - d_im) * c, (d_re + d_im) * c
        else:
            odd_re[k], odd_im[k] = d_re * c - d_im * s, d_re * s + d_im * c
    even_re[q], odd_re[q] = re[q], -im[q]
    out = [None] * n
    out[0::2] = half_spectrum_transposed(even_re, even_im)
    out[1::2] = half_spectrum_transposed(odd_re, odd_im)
    return out


def split(x):
    high = x.astype(bf16)
    return high, (x - high.astype(f32)).astype(bf16)


def dot(a, b):
    return jnp.dot(a, b, preferred_element_type=f32)


def dot_t(a, b):
    return lax.dot_general(a, b, (((1,), (1,)), ((), ())), preferred_element_type=f32)


def nothing():
    pass


def lanes(index, size):
    return pl.ds(pl.multiple_of(index * size, size), size)


def remote(src, dst, send, recv, device):
    return pltpu.make_async_remote_copy(
        src_ref=src, dst_ref=dst, send_sem=send, recv_sem=recv,
        device_id=(device,), device_id_type=MESH,
    )


def read(ref, lead, m):
    pieces = [ref[*lead, :, 2 * m + i].reshape(GRID, 128) for i in range(2)]
    return jnp.concatenate(pieces, axis=1)


def kernel(
    orb, kv, shell, left_in, four_in, forward_in, backward_in, total, margin,
    fields, work, screen, classes, left, four, forward, backward,
    w_high, w_low, v_high, v_low, grid_orb, grid_term, gram, rows, relay,
    load_sem, send_sem, recv_sem, part_send, part_recv, many_send, many_recv, meet_sem,
    relay_send, relay_recv,
):
    me = lax.axis_index("band")
    core = lax.rem(me, 2)
    x = lax.rem(me // 2, 4)
    plane = me // 8
    partner = me + 1 - 2 * core
    first = lax.rem(me + BANDS - 2 + 4 * core, BANDS)
    second = lax.rem(me + 2 - 4 * core + BANDS, BANDS)

    def wrap4(v):
        return lax.rem(v + 4, 4)

    def plane_at(dz, dy):
        return wrap4(plane // 4 + dz) * 4 + wrap4(plane + dy)

    load = pltpu.make_async_copy(orb, fields.at[0], load_sem.at[0])
    load.start()

    meetings = [partner]
    neighbours = [first, second] + [
        lax.rem(me + offset, BANDS) for offset in (6, 8, BANDS - 8, BANDS - 6)
    ]
    for scale in (2, 8, 32):
        here = lax.rem(me // scale, 4)
        base = me - here * scale
        meetings.append(me + scale * (1 - 2 * lax.rem(here, 2)))
        meetings.append(base + scale * (3 - here))
    barrier = pltpu.get_barrier_semaphore()
    for device in neighbours + meetings:
        pl.semaphore_signal(barrier, inc=1, device_id=(device,), device_id_type=MESH)
    small = [
        pltpu.make_async_copy(src, dst, load_sem.at[i + 1])
        for i, (src, dst) in enumerate(
            [(four_in, four), (forward_in, forward), (backward_in, backward),
             (left_in, left), (shell, classes)]
        )
    ]
    for copy in small:
        copy.start()
    pl.semaphore_wait(barrier, len(neighbours + meetings))
    load.wait()

    to_partner = remote(fields.at[0], fields.at[1], send_sem.at[0], recv_sem.at[0], partner)
    forward_on = remote(fields.at[2], fields.at[3], send_sem.at[1], recv_sem.at[1], partner)

    def send_field(slot, part, phase, device, below, crosses, relay_device):
        start = 2 * lax.rem(device // 2, 4) - below + 8

        def direct(i):
            group = lax.rem(start + i, 8)
            index = part if i < 3 else part + 1
            remote(
                fields.at[0, group], fields.at[slot, group],
                part_send.at[index], part_recv.at[index], device,
            ).start()

        @pl.when(crosses)
        def _():
            for i in range(RELAYED):
                remote(
                    fields.at[0, lax.rem(start + 8 - RELAYED + i, 8)],
                    relay.at[phase, i],
                    part_send.at[part + 1], relay_recv.at[phase], relay_device,
                ).start()

        for i in range(8 - RELAYED):
            direct(i)

        @pl.when(jnp.logical_not(crosses))
        def _():
            for i in range(8 - RELAYED, 8):
                direct(i)

    def pass_on(slot, part, phase, crosses):
        @pl.when(crosses)
        def _():
            up = x // 3
            device = lax.rem(me + 6 - 12 * up + BANDS, BANDS)
            below = (1 - core) if phase == 0 else core
            start = 2 * (3 - 3 * up) - below + 8
            for i in range(RELAYED):
                ref = relay.at[phase, pl.ds(0, RELAYED)]
                if i == 0:
                    remote(
                        ref, ref, relay_send.at[phase], relay_recv.at[phase], partner
                    ).wait_recv()
                remote(
                    relay.at[phase, i],
                    fields.at[slot, lax.rem(start + 8 - RELAYED + i, 8)],
                    relay_send.at[phase], part_recv.at[part + 1], device,
                ).start()

    def passed_on(phase, crosses):
        @pl.when(crosses)
        def _():
            ref = relay.at[phase, pl.ds(0, RELAYED)]
            remote(
                ref, ref, relay_send.at[phase], relay_recv.at[phase], partner
            ).wait_send()

    def wait_field(slot, part):
        count = 3 if part % 2 == 0 else 5
        ref = fields.at[slot, pl.ds(0, count)]
        return remote(ref, ref, part_send.at[part], part_recv.at[part], partner)

    first_crosses = x == 3 * core
    second_crosses = x == 3 - 3 * core
    send_field(
        2, 0, 0, first, 1 - core, first_crosses,
        lax.rem(me - 8 + 16 * core + BANDS, BANDS),
    )
    to_partner.start()

    def send_slice(slot, orbital, owner):
        remote(
            fields.at[slot, lax.rem(owner, 8), pl.ds(owner // 8 * 2, 2)],
            grid_orb.at[pl.ds(orbital * 2, 2)],
            many_send.at[0], many_recv.at[0], owner,
        ).start()

    def send_near(slot, orbital):
        def one(t, carry):
            there = lax.rem(plane + t // 2, 16)
            side = lax.rem(core + t, 2)
            send_slice(slot, orbital, there * 8 + x * 2 + side)
            return carry

        lax.fori_loop(1, 32, one, 0)
        grid_orb[pl.ds(orbital * 2, 2)] = fields[slot, lax.rem(me, 8), pl.ds(plane * 2, 2)]

    def send_across(slot, orbital, x_there, side):
        def one(t, carry):
            there = lax.rem(plane + t, 16)
            send_slice(slot, orbital, there * 8 + x_there * 2 + side)
            return carry

        lax.fori_loop(0, 16, one, 0)

    def meet(step):
        pl.semaphore_signal(
            meet_sem.at[step], inc=1, device_id=(meetings[step],), device_id_type=MESH
        )

    def met(step):
        pl.semaphore_wait(meet_sem.at[step], 1)

    def make_tables(k, carry):
        for q in range(4):
            rows_here = pl.ds(q * GRID, GRID)
            high, low = split(four[...] * forward[pl.ds(k * 4 + q, 1), :])
            w_high[k, rows_here, :] = high
            w_low[k, rows_here, :] = low
            high, low = split(four[...] * backward[pl.ds(k * 4 + q, 1), :])
            v_high[k, rows_here, :] = high
            v_low[k, rows_here, :] = low
        return carry

    for copy in small[:3]:
        copy.wait()
    meet(0)
    lax.fori_loop(0, TILES, make_tables, 0)
    met(0)

    for copy in small[3:]:
        copy.wait()
    values = [kv[i] * (-1.0 / GRID**3) for i in range(32)]

    def look_up(index):
        level = values
        bit = 1
        while len(level) > 1:
            picked = (index & bit) != 0
            level = [
                jnp.where(picked, level[i + 1], level[i]) for i in range(0, len(level), 2)
            ]
            bit *= 2
        return level[0]

    def make_screen(g, carry):
        here = lanes(g, 8)
        left_half = lax.broadcasted_iota(jnp.int32, (8, 128), 1) < GRID

        def chunk(i):
            return classes[here, pl.ds(i * 128, 128)]

        def turned(i):
            return pltpu.roll(chunk(i), GRID, 1)

        for k in range(TILES):
            if k == 0:
                pair = (
                    jnp.where(left_half, chunk(0), turned(16)),
                    jnp.where(left_half, chunk(8), turned(24)),
                )
                screen[here, pl.ds(0, 128)] = look_up(pair[0])
                screen[here, pl.ds(128, 128)] = look_up(pair[1])
                continue
            if k % 2 == 0:
                mixed = jnp.where(left_half, chunk(k // 2), turned((32 - k) // 2))
            else:
                mixed = jnp.where(left_half, turned((k - 1) // 2), chunk((31 - k) // 2))
            found = look_up(mixed)
            screen[here, pl.ds(k * 256, 128)] = found
            screen[here, pl.ds(k * 256 + 128, 128)] = found
        return carry

    for step in (1, 2):
        meet(step)
        lax.fori_loop(4 * step - 4, 4 * step, make_screen, 0)
        met(step)

    def left_pass(value):
        high, low = split(value)
        return dot(left[...], jnp.concatenate([high, high, low], axis=0))

    def right_pass(value, w, w_rest):
        high, low = split(value)
        both = dot(jnp.concatenate([high, low], axis=0), w)
        return both[:GRID] + both[GRID:] + dot(high, w_rest)

    def send_terms(j):
        def one(g, carry):
            owner = j * 8 + g

            @pl.when(owner != me)
            def _():
                remote(
                    total.at[g, pl.ds(j * 2, 2)],
                    grid_term.at[pl.ds(me * 2, 2)],
                    many_send.at[1], many_recv.at[1], owner,
                ).start()

            return carry

        lax.fori_loop(0, 8, one, 0)

    def one_pair(it, after=None):
        last = it == 4
        after = after or {}
        def first_stage(m, c):
            here = lanes(m, 256)
            work[:, here] = left_pass(read(fields, (0,), m) * read(fields, (it,), m))
            return c

        lax.fori_loop(0, 16, first_stage, 0, unroll=True)
        after.get(1, nothing)()

        def second_stage(g, c):
            here = lanes(g, 8)
            re, im = half_spectrum([work[here, pl.ds(n * 128, 128)] for n in range(32)])
            work[here, pl.ds(0, 128)] = re[0]
            work[here, pl.ds(128, 128)] = re[16]
            for k in range(1, 16):
                work[here, pl.ds(k * 256, 128)] = re[k]
                work[here, pl.ds(k * 256 + 128, 128)] = im[k]
            return c

        lax.fori_loop(0, 8, second_stage, 0)
        after.get(2, nothing)()

        def third_stage(k, c):
            here = lanes(k, 256)
            spectrum = right_pass(work[:, here], w_high[k], w_low[k])
            work[:, here] = right_pass(spectrum * screen[:, here], v_high[k], v_low[k])
            return c

        lax.fori_loop(0, 16, third_stage, 0, unroll=True)
        after.get(3, nothing)()

        def fourth_stage(g, c):
            here = lanes(g, 8)
            re = [work[here, pl.ds(0, 128)]]
            im = [None]
            for k in range(1, 16):
                re.append(work[here, pl.ds(k * 256, 128)])
                im.append(work[here, pl.ds(k * 256 + 128, 128)])
            re.append(work[here, pl.ds(128, 128)])
            im.append(None)
            out = half_spectrum_transposed(re, im)
            for n in range(32):
                work[here, pl.ds(n * 128, 128)] = out[n]
            return c

        lax.fori_loop(0, 8, fourth_stage, 0)
        after.get(4, nothing)()

        for start in range(0, 16, SENT_TOGETHER):
            for dz, dy in SHIFTS[start : start + SENT_TOGETHER]:
                j = plane_at(dz, dy)
                added = left_pass(work[:, lanes(j, 256)])
                for i in range(2):
                    part = added[:, i * 128 : i * 128 + 128].reshape(8, 8, 128)
                    term = part * fields[it, :, 2 * j + i]
                    if it == 0:
                        total[:, 2 * j + i] = term
                    else:
                        total[:, 2 * j + i] += term
            if last and start > 0:
                for shift in SHIFTS[start - SENT_TOGETHER : start]:
                    send_terms(plane_at(*shift))

    def next_step(step):
        met(step)
        meet(step + 1)

    def pass_orbital(slot, part, orbital, x_there, side):
        wait_field(slot, part).wait_recv()
        send_near(slot, orbital)
        send_across(slot, orbital, x_there, side)

    meet(3)
    one_pair(
        0,
        {1: lambda: next_step(3), 2: lambda: next_step(4), 3: lambda: next_step(5),
         4: lambda: met(6)},
    )
    pass_on(2, 0, 0, first_crosses)
    send_near(0, me)
    to_partner.wait_recv()
    one_pair(
        1, {2: lambda: pass_orbital(2, 0, second, wrap4(x - 1 + 2 * core), 1 - core)}
    )
    for part in range(2):
        wait_field(2, part).wait_send()
    send_field(
        4, 2, 1, second, core, second_crosses, lax.rem(me + 8 - 16 * core + BANDS, BANDS)
    )
    wait_field(2, 1).wait_recv()
    forward_on.start()
    one_pair(2)
    pass_on(4, 2, 1, second_crosses)
    forward_on.wait_recv()
    one_pair(
        3, {2: lambda: pass_orbital(4, 2, first, wrap4(x + 1 - 2 * core), core)}
    )
    wait_field(4, 3).wait_recv()
    one_pair(4)
    for shift in SHIFTS[16 - SENT_TOGETHER :]:
        send_terms(plane_at(*shift))
    grid_term[pl.ds(me * 2, 2)] = total[lax.rem(me, 8), pl.ds(plane * 2, 2)]

    def wait_many(count, buffer, index):
        part = buffer.at[pl.ds(0, count)]
        remote(part, part, many_send.at[index], many_recv.at[index], partner).wait_recv()

    wait_many(125 * 2, grid_orb, 0)
    wait_many(127 * 2, grid_term, 1)
    def across(buffer, s):
        flat = buffer.reshape(BANDS * 16, 128)
        return jnp.concatenate(
            [flat[pl.ds(8 * i + s, BANDS, stride=16), :] for i in range(2)], axis=1
        )

    result = jnp.zeros((BANDS, BANDS), f32)
    for s in range(8):
        a_high, a_low = split(across(grid_orb, s))
        b_high, b_low = split(across(grid_term, s))
        result += dot_t(a_high, b_high) + dot_t(a_low, b_high) + dot_t(a_high, b_low)
    result = result * (1.0 / GRID**3)
    for i in range(BANDS):
        gram[i] = result[i : i + 1, :]

    def send_row(t, carry):
        owner = lax.rem(me + t, BANDS)
        remote(
            gram.at[owner], rows.at[me], many_send.at[2], many_recv.at[2], owner
        ).start()
        return carry

    lax.fori_loop(1, BANDS, send_row, 0)
    rows[me] = gram[me]
    part = rows.at[pl.ds(0, BANDS - 1)]
    remote(part, part, many_send.at[2], many_recv.at[2], partner).wait_recv()
    margin[...] = jnp.sum(rows[...], axis=0)

    to_partner.wait_send()
    forward_on.wait_send()
    for part in range(2, 4):
        wait_field(4, part).wait_send()
    passed_on(0, first_crosses)
    passed_on(1, second_crosses)
    part = grid_orb.at[pl.ds(0, 125 * 2)]
    remote(part, part, many_send.at[0], many_recv.at[0], partner).wait_send()
    part = grid_term.at[pl.ds(0, 127 * 2)]
    remote(part, part, many_send.at[1], many_recv.at[1], partner).wait_send()
    part = rows.at[pl.ds(0, BANDS - 1)]
    remote(part, part, many_send.at[2], many_recv.at[2], partner).wait_send()


def finish(total, margin, exch, out, sem):
    copy = pltpu.make_async_copy(total, exch, sem)
    copy.start()
    out[...] = margin[...]
    copy.wait()


def local(orbitals, kernel_values, shell_index):
    any_space = pl.BlockSpec(memory_space=pl.ANY)
    hbm = pl.BlockSpec(memory_space=pltpu.HBM)
    vmem = pl.BlockSpec(memory_space=pltpu.VMEM)
    tables = constants()
    total, margin = pl.pallas_call(
        kernel,
        out_shape=(pltpu.VMEM(TILED, f32), pltpu.VMEM((1, BANDS), f32)),
        in_specs=[hbm, pl.BlockSpec(memory_space=pltpu.SMEM)] + [hbm] * 5,
        out_specs=(vmem, vmem),
        scratch_shapes=[
            pltpu.VMEM((5, *TILED), f32),
            pltpu.VMEM((GRID, WIDE), f32),
            pltpu.VMEM((GRID, WIDE), f32),
            pltpu.VMEM((GRID, WIDE), jnp.int32),
            *[pltpu.VMEM(t.shape, t.dtype) for t in tables],
            *[pltpu.VMEM((TILES, 256, 256), bf16)] * 4,
            pltpu.VMEM((BANDS * 2, 8, 128), f32),
            pltpu.VMEM((BANDS * 2, 8, 128), f32),
            pltpu.VMEM((BANDS, 1, BANDS), f32),
            pltpu.VMEM((BANDS, 1, BANDS), f32),
            pltpu.VMEM((2, RELAYED, *TILED[1:]), f32),
            pltpu.SemaphoreType.DMA((6,)),
            pltpu.SemaphoreType.DMA((2,)),
            pltpu.SemaphoreType.DMA((2,)),
            pltpu.SemaphoreType.DMA((4,)),
            pltpu.SemaphoreType.DMA((4,)),
            pltpu.SemaphoreType.DMA((3,)),
            pltpu.SemaphoreType.DMA((3,)),
            pltpu.SemaphoreType.REGULAR((7,)),
            pltpu.SemaphoreType.DMA((2,)),
            pltpu.SemaphoreType.DMA((2,)),
        ],
        compiler_params=pltpu.CompilerParams(
            collective_id=0, has_side_effects=True, vmem_limit_bytes=62 * 1024 * 1024 + 768 * 1024
        ),
        name="exchange",
    )(
        orbitals.reshape(8, 8, 32, 128).transpose(0, 2, 1, 3),
        kernel_values,
        shell_index,
        *[jnp.asarray(c) for c in tables],
    )
    exchange, margin = pl.pallas_call(
        finish,
        out_shape=(
            jax.ShapeDtypeStruct(TILED, f32),
            jax.ShapeDtypeStruct((1, BANDS), f32),
        ),
        in_specs=[vmem, vmem],
        out_specs=(any_space, vmem),
        scratch_shapes=[pltpu.SemaphoreType.DMA],
        name="finish",
    )(
        pltpu.with_memory_space_constraint(total, pltpu.VMEM),
        pltpu.with_memory_space_constraint(margin, pltpu.VMEM),
    )
    return exchange.transpose(0, 2, 1, 3).reshape(1, GRID, WIDE), margin


def solution(mesh):
    return jax.shard_map(
        local,
        mesh=mesh,
        in_specs=(P("band", None, None), P(), P()),
        out_specs=(P("band", None, None), P("band", None)),
        check_vma=False,
    )
```

```python
import math

import jax
import jax.numpy as jnp
import numpy as np
from jax import lax
from jax.experimental import pallas as pl
from jax.experimental.pallas import tpu as pltpu
from jax.sharding import PartitionSpec as P

GRID = 64
WIDE = GRID * GRID
BANDS = 128
TILES = 16
SENT_TOGETHER = 4
TILED = (8, 32, 8, 128)
SHIFTS = sorted(
    ((dz, dy) for dz in range(4) for dy in range(4)),
    key=lambda s: -min(s[0], 4 - s[0]) - min(s[1], 4 - s[1]),
)
MESH = pl.DeviceIdType.MESH
f32 = jnp.float32
bf16 = jnp.bfloat16


def cas(angle):
    return math.cos(angle) + math.sin(angle)


def cas_table():
    index = np.arange(GRID)
    angle = 2.0 * math.pi / GRID * (index[:, None] * index[None] % GRID)
    return np.cos(angle) + np.sin(angle)


def frequencies(k):
    return (0, 32, 16, 48) if k == 0 else (k, 32 - k, 64 - k, 32 + k)


def mixing(k):
    table = np.zeros((4, 4))
    for t, b in enumerate(frequencies(k)):
        for q in range(4):
            part, r = q // 2, q % 2
            angle = 2.0 * math.pi * b * r / GRID
            if k == 0:
                table[q, t] = cas(angle) if (part == 0) == (b % 32 == 0) else 0.0
            elif part == 0:
                table[q, t] = cas(angle)
            else:
                sign = 1.0 if b in (k, 32 + k) else -1.0
                table[q, t] = sign * (math.sin(angle) - math.cos(angle))
    return table


def constants():
    table = cas_table()
    high = table.astype(np.float32).astype(bf16)
    low = (table - high.astype(np.float64)).astype(np.float32).astype(bf16)
    left = np.concatenate([high, low, high], axis=1)
    four = np.tile(table, (1, 4)).astype(np.float32)
    mixes = np.stack([mixing(k) for k in range(TILES)])
    forward = np.repeat(mixes.reshape(TILES * 4, 4), GRID, axis=1).astype(np.float32)
    backward = np.repeat(
        np.swapaxes(mixes, 1, 2).reshape(TILES * 4, 4), GRID, axis=1
    ).astype(np.float32)
    return left, four, forward, backward


def half_spectrum(xs):
    n = len(xs)
    if n == 2:
        return [xs[0] + xs[1], xs[0] - xs[1]], [None, None]
    even_re, even_im = half_spectrum(xs[0::2])
    odd_re, odd_im = half_spectrum(xs[1::2])
    h, q = n // 2, n // 4
    re, im = [None] * (h + 1), [None] * (h + 1)
    re[0], re[h] = even_re[0] + odd_re[0], even_re[0] - odd_re[0]
    for k in range(1, q):
        c, s = math.cos(2 * math.pi * k / n), -math.sin(2 * math.pi * k / n)
        if 2 * k == q:
            t_re, t_im = (odd_re[k] + odd_im[k]) * c, (odd_im[k] - odd_re[k]) * c
        else:
            t_re = odd_re[k] * c - odd_im[k] * s
            t_im = odd_re[k] * s + odd_im[k] * c
        re[k], im[k] = even_re[k] + t_re, even_im[k] + t_im
        re[h - k], im[h - k] = even_re[k] - t_re, t_im - even_im[k]
    re[q], im[q] = even_re[q], -odd_re[q]
    return re, im


def half_spectrum_transposed(re, im):
    h = len(re) - 1
    n = 2 * h
    if n == 2:
        return [re[0] + re[1], re[0] - re[1]]
    q = n // 4
    even_re, even_im = [None] * (q + 1), [None] * (q + 1)
    odd_re, odd_im = [None] * (q + 1), [None] * (q + 1)
    even_re[0], odd_re[0] = re[0] + re[h], re[0] - re[h]
    for k in range(1, q):
        even_re[k], even_im[k] = re[k] + re[h - k], im[k] - im[h - k]
        d_re, d_im = re[k] - re[h - k], im[k] + im[h - k]
        c, s = math.cos(2 * math.pi * k / n), math.sin(2 * math.pi * k / n)
        if 2 * k == q:
            odd_re[k], odd_im[k] = (d_re - d_im) * c, (d_re + d_im) * c
        else:
            odd_re[k], odd_im[k] = d_re * c - d_im * s, d_re * s + d_im * c
    even_re[q], odd_re[q] = re[q], -im[q]
    out = [None] * n
    out[0::2] = half_spectrum_transposed(even_re, even_im)
    out[1::2] = half_spectrum_transposed(odd_re, odd_im)
    return out


def split(x):
    high = x.astype(bf16)
    return high, (x - high.astype(f32)).astype(bf16)


def dot(a, b):
    return jnp.dot(a, b, preferred_element_type=f32)


def dot_t(a, b):
    return lax.dot_general(a, b, (((1,), (1,)), ((), ())), preferred_element_type=f32)


def nothing():
    pass


def lanes(index, size):
    return pl.ds(pl.multiple_of(index * size, size), size)


def remote(src, dst, send, recv, device):
    return pltpu.make_async_remote_copy(
        src_ref=src, dst_ref=dst, send_sem=send, recv_sem=recv,
        device_id=(device,), device_id_type=MESH,
    )


def read(ref, lead, m):
    pieces = [ref[*lead, :, 2 * m + i].reshape(GRID, 128) for i in range(2)]
    return jnp.concatenate(pieces, axis=1)


def kernel(
    orb, kv, shell, left_in, four_in, forward_in, backward_in, total, margin,
    fields, work, screen, classes, left, four, forward, backward,
    w_high, w_low, v_high, v_low, grid_orb, grid_term, gram, rows, relay,
    load_sem, send_sem, recv_sem, part_send, part_recv, many_send, many_recv, meet_sem,
    relay_send, relay_recv,
):
    me = lax.axis_index("band")
    core = lax.rem(me, 2)
    x = lax.rem(me // 2, 4)
    plane = me // 8
    partner = me + 1 - 2 * core
    first = lax.rem(me + BANDS - 2 + 4 * core, BANDS)
    second = lax.rem(me + 2 - 4 * core + BANDS, BANDS)

    def wrap4(v):
        return lax.rem(v + 4, 4)

    def plane_at(dz, dy):
        return wrap4(plane // 4 + dz) * 4 + wrap4(plane + dy)

    load = pltpu.make_async_copy(orb, fields.at[0], load_sem.at[0])
    load.start()

    meetings = [partner]
    neighbours = [first, second, lax.rem(me + 8, BANDS), lax.rem(me + BANDS - 8, BANDS)]
    for scale in (2, 8, 32):
        here = lax.rem(me // scale, 4)
        base = me - here * scale
        meetings.append(me + scale * (1 - 2 * lax.rem(here, 2)))
        meetings.append(base + scale * (3 - here))
    barrier = pltpu.get_barrier_semaphore()
    for device in neighbours + meetings:
        pl.semaphore_signal(barrier, inc=1, device_id=(device,), device_id_type=MESH)
    small = [
        pltpu.make_async_copy(src, dst, load_sem.at[i + 1])
        for i, (src, dst) in enumerate(
            [(four_in, four), (forward_in, forward), (backward_in, backward),
             (left_in, left), (shell, classes)]
        )
    ]
    for copy in small:
        copy.start()
    pl.semaphore_wait(barrier, len(neighbours + meetings))
    load.wait()

    to_partner = remote(fields.at[0], fields.at[1], send_sem.at[0], recv_sem.at[0], partner)
    forward_on = remote(fields.at[2], fields.at[3], send_sem.at[1], recv_sem.at[1], partner)

    def send_groups(source, target, device_x, below, send, recv, part, device):
        start = 2 * device_x - below + 8
        for i in range(8):
            group = lax.rem(start + i, 8)
            index = part if i < 3 else part + 1
            remote(source(i, group), target(i, group), send(index), recv(index), device).start()

    def send_field(slot, part, device, below):
        send_groups(
            lambda i, group: fields.at[0, group], lambda i, group: fields.at[slot, group],
            lax.rem(device // 2, 4), below,
            lambda index: part_send.at[index], lambda index: part_recv.at[index],
            part, device,
        )

    second_crosses = x == 3 - 3 * core

    def send_ahead():
        send_groups(
            lambda i, group: fields.at[0, group], lambda i, group: relay.at[i],
            lax.rem(second // 2, 4), core,
            lambda index: part_send.at[index], lambda index: relay_recv.at[index - 2],
            2, lax.rem(me + 8 - 16 * core + BANDS, BANDS),
        )

    def pass_on():
        up = x // 3
        device = lax.rem(me + 6 - 12 * up + BANDS, BANDS)
        for part, groups in ((0, range(3)), (1, range(3, 8))):
            ref = relay.at[pl.ds(0, len(groups))]
            remote(ref, ref, relay_send, relay_recv.at[part], partner).wait_recv()
            for i in groups:
                remote(
                    relay.at[i],
                    fields.at[4, lax.rem(2 * (3 - 3 * up) - core + 8 + i, 8)],
                    relay_send, part_recv.at[2 + part], device,
                ).start()

    def passed_on():
        @pl.when(second_crosses)
        def _():
            remote(relay, relay, relay_send, relay_recv.at[0], partner).wait_send()

    def wait_field(slot, part):
        count = 3 if part % 2 == 0 else 5
        ref = fields.at[slot, pl.ds(0, count)]
        return remote(ref, ref, part_send.at[part], part_recv.at[part], partner)

    send_field(2, 0, first, 1 - core)
    pl.when(second_crosses)(send_ahead)
    to_partner.start()

    def send_slice(slot, orbital, owner):
        remote(
            fields.at[slot, lax.rem(owner, 8), pl.ds(owner // 8 * 2, 2)],
            grid_orb.at[pl.ds(orbital * 2, 2)],
            many_send.at[0], many_recv.at[0], owner,
        ).start()

    def send_near(slot, orbital):
        def one(t, carry):
            there = lax.rem(plane + t // 2, 16)
            side = lax.rem(core + t, 2)
            send_slice(slot, orbital, there * 8 + x * 2 + side)
            return carry

        lax.fori_loop(1, 32, one, 0)
        grid_orb[pl.ds(orbital * 2, 2)] = fields[slot, lax.rem(me, 8), pl.ds(plane * 2, 2)]

    def send_across(slot, orbital, x_there, side):
        def one(t, carry):
            there = lax.rem(plane + t, 16)
            send_slice(slot, orbital, there * 8 + x_there * 2 + side)
            return carry

        lax.fori_loop(0, 16, one, 0)

    def meet(step):
        pl.semaphore_signal(
            meet_sem.at[step], inc=1, device_id=(meetings[step],), device_id_type=MESH
        )

    def met(step):
        pl.semaphore_wait(meet_sem.at[step], 1)

    def make_tables(k, carry):
        for q in range(4):
            rows_here = pl.ds(q * GRID, GRID)
            high, low = split(four[...] * forward[pl.ds(k * 4 + q, 1), :])
            w_high[k, rows_here, :] = high
            w_low[k, rows_here, :] = low
            high, low = split(four[...] * backward[pl.ds(k * 4 + q, 1), :])
            v_high[k, rows_here, :] = high
            v_low[k, rows_here, :] = low
        return carry

    for copy in small[:3]:
        copy.wait()
    meet(0)
    lax.fori_loop(0, TILES, make_tables, 0)
    met(0)

    for copy in small[3:]:
        copy.wait()
    values = [kv[i] * (-1.0 / GRID**3) for i in range(32)]

    def look_up(index):
        level = values
        bit = 1
        while len(level) > 1:
            picked = (index & bit) != 0
            level = [
                jnp.where(picked, level[i + 1], level[i]) for i in range(0, len(level), 2)
            ]
            bit *= 2
        return level[0]

    def make_screen(g, carry):
        here = lanes(g, 8)
        left_half = lax.broadcasted_iota(jnp.int32, (8, 128), 1) < GRID

        def chunk(i):
            return classes[here, pl.ds(i * 128, 128)]

        def turned(i):
            return pltpu.roll(chunk(i), GRID, 1)

        for k in range(TILES):
            if k == 0:
                pair = (
                    jnp.where(left_half, chunk(0), turned(16)),
                    jnp.where(left_half, chunk(8), turned(24)),
                )
                screen[here, pl.ds(0, 128)] = look_up(pair[0])
                screen[here, pl.ds(128, 128)] = look_up(pair[1])
                continue
            if k % 2 == 0:
                mixed = jnp.where(left_half, chunk(k // 2), turned((32 - k) // 2))
            else:
                mixed = jnp.where(left_half, turned((k - 1) // 2), chunk((31 - k) // 2))
            found = look_up(mixed)
            screen[here, pl.ds(k * 256, 128)] = found
            screen[here, pl.ds(k * 256 + 128, 128)] = found
        return carry

    for step in (1, 2):
        meet(step)
        lax.fori_loop(4 * step - 4, 4 * step, make_screen, 0)
        met(step)

    def left_pass(value):
        high, low = split(value)
        return dot(left[...], jnp.concatenate([high, high, low], axis=0))

    def right_pass(value, w, w_rest):
        high, low = split(value)
        both = dot(jnp.concatenate([high, low], axis=0), w)
        return both[:GRID] + both[GRID:] + dot(high, w_rest)

    def in_plane(shift):
        j = plane_at(*shift)
        for dx in (2, 1, 3, 0):
            for side in (1, 0):
                if shift != (0, 0) or dx != 0 or side != 0:
                    yield j * 8 + wrap4(x + dx) * 2 + lax.rem(core + side, 2)

    def send_terms(shift):
        for owner in in_plane(shift):
            remote(
                total.at[lax.rem(owner, 8), pl.ds(owner // 8 * 2, 2)],
                grid_term.at[pl.ds(me * 2, 2)],
                many_send.at[1], many_recv.at[1], owner,
            ).start()

    def one_pair(it, after=None):
        last = it == 4
        after = after or {}
        def first_stage(m, c):
            here = lanes(m, 256)
            work[:, here] = left_pass(read(fields, (0,), m) * read(fields, (it,), m))
            return c

        lax.fori_loop(0, 16, first_stage, 0, unroll=True)
        after.get(1, nothing)()

        def second_stage(g, c):
            here = lanes(g, 8)
            re, im = half_spectrum([work[here, pl.ds(n * 128, 128)] for n in range(32)])
            work[here, pl.ds(0, 128)] = re[0]
            work[here, pl.ds(128, 128)] = re[16]
            for k in range(1, 16):
                work[here, pl.ds(k * 256, 128)] = re[k]
                work[here, pl.ds(k * 256 + 128, 128)] = im[k]
            return c

        lax.fori_loop(0, 8, second_stage, 0)
        after.get(2, nothing)()

        def third_stage(k, c):
            here = lanes(k, 256)
            spectrum = right_pass(work[:, here], w_high[k], w_low[k])
            work[:, here] = right_pass(spectrum * screen[:, here], v_high[k], v_low[k])
            return c

        lax.fori_loop(0, 16, third_stage, 0, unroll=True)
        after.get(3, nothing)()

        def fourth_stage(g, c):
            here = lanes(g, 8)
            re = [work[here, pl.ds(0, 128)]]
            im = [None]
            for k in range(1, 16):
                re.append(work[here, pl.ds(k * 256, 128)])
                im.append(work[here, pl.ds(k * 256 + 128, 128)])
            re.append(work[here, pl.ds(128, 128)])
            im.append(None)
            out = half_spectrum_transposed(re, im)
            for n in range(32):
                work[here, pl.ds(n * 128, 128)] = out[n]
            return c

        lax.fori_loop(0, 8, fourth_stage, 0)
        after.get(4, nothing)()

        for start in range(0, 16, SENT_TOGETHER):
            for dz, dy in SHIFTS[start : start + SENT_TOGETHER]:
                j = plane_at(dz, dy)
                added = left_pass(work[:, lanes(j, 256)])
                for i in range(2):
                    part = added[:, i * 128 : i * 128 + 128].reshape(8, 8, 128)
                    term = part * fields[it, :, 2 * j + i]
                    if it == 0:
                        total[:, 2 * j + i] = term
                    else:
                        total[:, 2 * j + i] += term
            if last and start > 0:
                for shift in SHIFTS[start - SENT_TOGETHER : start]:
                    send_terms(shift)

    def next_step(step):
        met(step)
        meet(step + 1)

    def pass_orbital(slot, part, orbital, x_there, side):
        wait_field(slot, part).wait_recv()
        send_near(slot, orbital)
        send_across(slot, orbital, x_there, side)

    meet(3)
    one_pair(
        0,
        {1: lambda: next_step(3), 2: lambda: next_step(4), 3: lambda: next_step(5),
         4: lambda: met(6)},
    )
    to_partner.wait_recv()

    def fetch_second():
        for part in range(2):
            wait_field(2, part).wait_send()
        pl.when(second_crosses)(pass_on)
        pl.when(jnp.logical_not(second_crosses))(lambda: send_field(4, 2, second, core))

    one_pair(
        1,
        {1: fetch_second,
         3: lambda: (
             send_near(0, me),
             pass_orbital(2, 0, second, wrap4(x - 1 + 2 * core), 1 - core),
         )},
    )
    wait_field(2, 1).wait_recv()
    forward_on.start()
    one_pair(2)
    forward_on.wait_recv()
    one_pair(
        3, {2: lambda: pass_orbital(4, 2, first, wrap4(x + 1 - 2 * core), core)}
    )
    wait_field(4, 3).wait_recv()
    one_pair(4)
    for shift in SHIFTS[16 - SENT_TOGETHER :]:
        send_terms(shift)
    grid_term[pl.ds(me * 2, 2)] = total[lax.rem(me, 8), pl.ds(plane * 2, 2)]

    def wait_many(count, buffer, index):
        part = buffer.at[pl.ds(0, count)]
        remote(part, part, many_send.at[index], many_recv.at[index], partner).wait_recv()

    wait_many(125 * 2, grid_orb, 0)
    wait_many(127 * 2, grid_term, 1)
    def across(buffer, s):
        flat = buffer.reshape(BANDS * 16, 128)
        return jnp.concatenate(
            [flat[pl.ds(8 * i + s, BANDS, stride=16), :] for i in range(2)], axis=1
        )

    result = jnp.zeros((BANDS, BANDS), f32)
    for s in range(8):
        a_high, a_low = split(across(grid_orb, s))
        b_high, b_low = split(across(grid_term, s))
        result += dot_t(a_high, b_high) + dot_t(a_low, b_high) + dot_t(a_high, b_low)
    result = result * (1.0 / GRID**3)
    for i in range(BANDS):
        gram[i] = result[i : i + 1, :]

    for shift in SHIFTS:
        for owner in in_plane(shift):
            remote(
                gram.at[owner], rows.at[me], many_send.at[2], many_recv.at[2], owner
            ).start()
    rows[me] = gram[me]
    part = rows.at[pl.ds(0, BANDS - 1)]
    remote(part, part, many_send.at[2], many_recv.at[2], partner).wait_recv()
    margin[...] = jnp.sum(rows[...], axis=0)

    to_partner.wait_send()
    forward_on.wait_send()
    for part in range(2, 4):
        wait_field(4, part).wait_send()
    passed_on()
    part = grid_orb.at[pl.ds(0, 125 * 2)]
    remote(part, part, many_send.at[0], many_recv.at[0], partner).wait_send()
    part = grid_term.at[pl.ds(0, 127 * 2)]
    remote(part, part, many_send.at[1], many_recv.at[1], partner).wait_send()
    part = rows.at[pl.ds(0, BANDS - 1)]
    remote(part, part, many_send.at[2], many_recv.at[2], partner).wait_send()


def finish(total, margin, exch, out, sem):
    copy = pltpu.make_async_copy(total, exch, sem)
    copy.start()
    out[...] = margin[...]
    copy.wait()


def local(orbitals, kernel_values, shell_index):
    any_space = pl.BlockSpec(memory_space=pl.ANY)
    hbm = pl.BlockSpec(memory_space=pltpu.HBM)
    vmem = pl.BlockSpec(memory_space=pltpu.VMEM)
    tables = constants()
    total, margin = pl.pallas_call(
        kernel,
        out_shape=(pltpu.VMEM(TILED, f32), pltpu.VMEM((1, BANDS), f32)),
        in_specs=[hbm, pl.BlockSpec(memory_space=pltpu.SMEM)] + [hbm] * 5,
        out_specs=(vmem, vmem),
        scratch_shapes=[
            pltpu.VMEM((5, *TILED), f32),
            pltpu.VMEM((GRID, WIDE), f32),
            pltpu.VMEM((GRID, WIDE), f32),
            pltpu.VMEM((GRID, WIDE), jnp.int32),
            *[pltpu.VMEM(t.shape, t.dtype) for t in tables],
            *[pltpu.VMEM((TILES, 256, 256), bf16)] * 4,
            pltpu.VMEM((BANDS * 2, 8, 128), f32),
            pltpu.VMEM((BANDS * 2, 8, 128), f32),
            pltpu.VMEM((BANDS, 1, BANDS), f32),
            pltpu.VMEM((BANDS, 1, BANDS), f32),
            pltpu.VMEM(TILED, f32),
            pltpu.SemaphoreType.DMA((6,)),
            pltpu.SemaphoreType.DMA((2,)),
            pltpu.SemaphoreType.DMA((2,)),
            pltpu.SemaphoreType.DMA((4,)),
            pltpu.SemaphoreType.DMA((4,)),
            pltpu.SemaphoreType.DMA((3,)),
            pltpu.SemaphoreType.DMA((3,)),
            pltpu.SemaphoreType.REGULAR((7,)),
            pltpu.SemaphoreType.DMA,
            pltpu.SemaphoreType.DMA((2,)),
        ],
        compiler_params=pltpu.CompilerParams(
            collective_id=0, has_side_effects=True, vmem_limit_bytes=62 * 1024 * 1024 + 768 * 1024
        ),
        name="exchange",
    )(
        orbitals.reshape(8, 8, 32, 128).transpose(0, 2, 1, 3),
        kernel_values,
        shell_index,
        *[jnp.asarray(c) for c in tables],
    )
    exchange, margin = pl.pallas_call(
        finish,
        out_shape=(
            jax.ShapeDtypeStruct(TILED, f32),
            jax.ShapeDtypeStruct((1, BANDS), f32),
        ),
        in_specs=[vmem, vmem],
        out_specs=(any_space, vmem),
        scratch_shapes=[pltpu.SemaphoreType.DMA],
        name="finish",
    )(
        pltpu.with_memory_space_constraint(total, pltpu.VMEM),
        pltpu.with_memory_space_constraint(margin, pltpu.VMEM),
    )
    return exchange.transpose(0, 2, 1, 3).reshape(1, GRID, WIDE), margin


def solution(mesh):
    return jax.shard_map(
        local,
        mesh=mesh,
        in_specs=(P("band", None, None), P(), P()),
        out_specs=(P("band", None, None), P("band", None)),
        check_vma=False,
    )
```

```python
import math

import jax
import jax.numpy as jnp
import numpy as np
from jax import lax
from jax.experimental import pallas as pl
from jax.experimental.pallas import tpu as pltpu
from jax.sharding import PartitionSpec as P

GRID = 64
WIDE = GRID * GRID
BANDS = 128
TILES = 16
SENT_TOGETHER = 2
TILED = (8, 32, 8, 128)
SHIFTS = sorted(
    ((dz, dy) for dz in range(4) for dy in range(4)),
    key=lambda s: -min(s[0], 4 - s[0]) - min(s[1], 4 - s[1]),
)
MESH = pl.DeviceIdType.MESH
f32 = jnp.float32
bf16 = jnp.bfloat16


def cas(angle):
    return math.cos(angle) + math.sin(angle)


def cas_table():
    index = np.arange(GRID)
    angle = 2.0 * math.pi / GRID * (index[:, None] * index[None] % GRID)
    return np.cos(angle) + np.sin(angle)


def frequencies(k):
    return (0, 32, 16, 48) if k == 0 else (k, 32 - k, 64 - k, 32 + k)


def mixing(k):
    table = np.zeros((4, 4))
    for t, b in enumerate(frequencies(k)):
        for q in range(4):
            part, r = q // 2, q % 2
            angle = 2.0 * math.pi * b * r / GRID
            if k == 0:
                table[q, t] = cas(angle) if (part == 0) == (b % 32 == 0) else 0.0
            elif part == 0:
                table[q, t] = cas(angle)
            else:
                sign = 1.0 if b in (k, 32 + k) else -1.0
                table[q, t] = sign * (math.sin(angle) - math.cos(angle))
    return table


def constants():
    table = cas_table()
    high = table.astype(np.float32).astype(bf16)
    low = (table - high.astype(np.float64)).astype(np.float32).astype(bf16)
    left = np.concatenate([high, low, high], axis=1)
    four = np.tile(table, (1, 4)).astype(np.float32)
    mixes = np.stack([mixing(k) for k in range(TILES)])
    forward = np.repeat(mixes.reshape(TILES * 4, 4), GRID, axis=1).astype(np.float32)
    backward = np.repeat(
        np.swapaxes(mixes, 1, 2).reshape(TILES * 4, 4), GRID, axis=1
    ).astype(np.float32)
    return left, four, forward, backward


def half_spectrum(xs):
    n = len(xs)
    if n == 2:
        return [xs[0] + xs[1], xs[0] - xs[1]], [None, None]
    even_re, even_im = half_spectrum(xs[0::2])
    odd_re, odd_im = half_spectrum(xs[1::2])
    h, q = n // 2, n // 4
    re, im = [None] * (h + 1), [None] * (h + 1)
    re[0], re[h] = even_re[0] + odd_re[0], even_re[0] - odd_re[0]
    for k in range(1, q):
        c, s = math.cos(2 * math.pi * k / n), -math.sin(2 * math.pi * k / n)
        if 2 * k == q:
            t_re, t_im = (odd_re[k] + odd_im[k]) * c, (odd_im[k] - odd_re[k]) * c
        else:
            t_re = odd_re[k] * c - odd_im[k] * s
            t_im = odd_re[k] * s + odd_im[k] * c
        re[k], im[k] = even_re[k] + t_re, even_im[k] + t_im
        re[h - k], im[h - k] = even_re[k] - t_re, t_im - even_im[k]
    re[q], im[q] = even_re[q], -odd_re[q]
    return re, im


def half_spectrum_transposed(re, im):
    h = len(re) - 1
    n = 2 * h
    if n == 2:
        return [re[0] + re[1], re[0] - re[1]]
    q = n // 4
    even_re, even_im = [None] * (q + 1), [None] * (q + 1)
    odd_re, odd_im = [None] * (q + 1), [None] * (q + 1)
    even_re[0], odd_re[0] = re[0] + re[h], re[0] - re[h]
    for k in range(1, q):
        even_re[k], even_im[k] = re[k] + re[h - k], im[k] - im[h - k]
        d_re, d_im = re[k] - re[h - k], im[k] + im[h - k]
        c, s = math.cos(2 * math.pi * k / n), math.sin(2 * math.pi * k / n)
        if 2 * k == q:
            odd_re[k], odd_im[k] = (d_re - d_im) * c, (d_re + d_im) * c
        else:
            odd_re[k], odd_im[k] = d_re * c - d_im * s, d_re * s + d_im * c
    even_re[q], odd_re[q] = re[q], -im[q]
    out = [None] * n
    out[0::2] = half_spectrum_transposed(even_re, even_im)
    out[1::2] = half_spectrum_transposed(odd_re, odd_im)
    return out


def split(x):
    high = x.astype(bf16)
    return high, (x - high.astype(f32)).astype(bf16)


def dot(a, b):
    return jnp.dot(a, b, preferred_element_type=f32)


def dot_t(a, b):
    return lax.dot_general(a, b, (((1,), (1,)), ((), ())), preferred_element_type=f32)


def nothing():
    pass


def lanes(index, size):
    return pl.ds(pl.multiple_of(index * size, size), size)


def remote(src, dst, send, recv, device):
    return pltpu.make_async_remote_copy(
        src_ref=src, dst_ref=dst, send_sem=send, recv_sem=recv,
        device_id=(device,), device_id_type=MESH,
    )


def read(ref, lead, m):
    pieces = [ref[*lead, :, 2 * m + i].reshape(GRID, 128) for i in range(2)]
    return jnp.concatenate(pieces, axis=1)


def kernel(
    orb, kv, shell, left_in, four_in, forward_in, backward_in, total, margin,
    fields, work, screen, classes, left, four, forward, backward,
    w_high, w_low, v_high, v_low, grid_orb, grid_term, gram, rows, relay,
    orb_high, orb_low,
    load_sem, send_sem, recv_sem, part_send, part_recv, many_send, many_recv, meet_sem,
    relay_send, relay_recv,
):
    me = lax.axis_index("band")
    core = lax.rem(me, 2)
    x = lax.rem(me // 2, 4)
    plane = me // 8
    partner = me + 1 - 2 * core
    first = lax.rem(me + BANDS - 2 + 4 * core, BANDS)
    second = lax.rem(me + 2 - 4 * core + BANDS, BANDS)

    def wrap4(v):
        return lax.rem(v + 4, 4)

    def plane_at(dz, dy):
        return wrap4(plane // 4 + dz) * 4 + wrap4(plane + dy)

    load = pltpu.make_async_copy(orb, fields.at[0], load_sem.at[0])
    load.start()

    meetings = [partner]
    neighbours = [first, second, lax.rem(me + 8, BANDS), lax.rem(me + BANDS - 8, BANDS)]
    for scale in (2, 8, 32):
        here = lax.rem(me // scale, 4)
        base = me - here * scale
        meetings.append(me + scale * (1 - 2 * lax.rem(here, 2)))
        meetings.append(base + scale * (3 - here))
    barrier = pltpu.get_barrier_semaphore()
    for device in neighbours + meetings:
        pl.semaphore_signal(barrier, inc=1, device_id=(device,), device_id_type=MESH)
    small = [
        pltpu.make_async_copy(src, dst, load_sem.at[i + 1])
        for i, (src, dst) in enumerate(
            [(four_in, four), (forward_in, forward), (backward_in, backward),
             (left_in, left), (shell, classes)]
        )
    ]
    for copy in small:
        copy.start()
    pl.semaphore_wait(barrier, len(neighbours + meetings))
    load.wait()

    to_partner = remote(fields.at[0], fields.at[1], send_sem.at[0], recv_sem.at[0], partner)
    forward_on = remote(fields.at[2], fields.at[3], send_sem.at[1], recv_sem.at[1], partner)

    def send_groups(source, target, device_x, below, send, recv, part, device):
        start = 2 * device_x - below + 8
        for i in range(8):
            group = lax.rem(start + i, 8)
            index = part if i < 3 else part + 1
            remote(source(i, group), target(i, group), send(index), recv(index), device).start()

    def send_field(slot, part, device, below):
        send_groups(
            lambda i, group: fields.at[0, group], lambda i, group: fields.at[slot, group],
            lax.rem(device // 2, 4), below,
            lambda index: part_send.at[index], lambda index: part_recv.at[index],
            part, device,
        )

    second_crosses = x == 3 - 3 * core

    def send_ahead():
        send_groups(
            lambda i, group: fields.at[0, group], lambda i, group: relay.at[i],
            lax.rem(second // 2, 4), core,
            lambda index: part_send.at[index], lambda index: relay_recv.at[index - 2],
            2, lax.rem(me + 8 - 16 * core + BANDS, BANDS),
        )

    def pass_on():
        up = x // 3
        device = lax.rem(me + 6 - 12 * up + BANDS, BANDS)
        for part, groups in ((0, range(3)), (1, range(3, 8))):
            ref = relay.at[pl.ds(0, len(groups))]
            remote(ref, ref, relay_send, relay_recv.at[part], partner).wait_recv()
            for i in groups:
                remote(
                    relay.at[i],
                    fields.at[4, lax.rem(2 * (3 - 3 * up) - core + 8 + i, 8)],
                    relay_send, part_recv.at[2 + part], device,
                ).start()

    def passed_on():
        @pl.when(second_crosses)
        def _():
            remote(relay, relay, relay_send, relay_recv.at[0], partner).wait_send()

    def wait_field(slot, part):
        count = 3 if part % 2 == 0 else 5
        ref = fields.at[slot, pl.ds(0, count)]
        return remote(ref, ref, part_send.at[part], part_recv.at[part], partner)

    send_field(2, 0, first, 1 - core)
    pl.when(second_crosses)(send_ahead)
    to_partner.start()

    def send_slice(slot, orbital, owner):
        remote(
            fields.at[slot, lax.rem(owner, 8), pl.ds(owner // 8 * 2, 2)],
            grid_orb.at[pl.ds(orbital * 2, 2)],
            many_send.at[0], many_recv.at[0], owner,
        ).start()

    def send_near(slot, orbital):
        def one(t, carry):
            there = lax.rem(plane + t // 2, 16)
            side = lax.rem(core + t, 2)
            send_slice(slot, orbital, there * 8 + x * 2 + side)
            return carry

        lax.fori_loop(1, 32, one, 0)
        grid_orb[pl.ds(orbital * 2, 2)] = fields[slot, lax.rem(me, 8), pl.ds(plane * 2, 2)]

    def send_across(slot, orbital, x_there, side):
        def one(t, carry):
            there = lax.rem(plane + t, 16)
            send_slice(slot, orbital, there * 8 + x_there * 2 + side)
            return carry

        lax.fori_loop(0, 16, one, 0)

    def meet(step):
        pl.semaphore_signal(
            meet_sem.at[step], inc=1, device_id=(meetings[step],), device_id_type=MESH
        )

    def met(step):
        pl.semaphore_wait(meet_sem.at[step], 1)

    def make_tables(k, carry):
        for q in range(4):
            rows_here = pl.ds(q * GRID, GRID)
            high, low = split(four[...] * forward[pl.ds(k * 4 + q, 1), :])
            w_high[k, rows_here, :] = high
            w_low[k, rows_here, :] = low
            high, low = split(four[...] * backward[pl.ds(k * 4 + q, 1), :])
            v_high[k, rows_here, :] = high
            v_low[k, rows_here, :] = low
        return carry

    for copy in small[:3]:
        copy.wait()
    meet(0)
    lax.fori_loop(0, TILES, make_tables, 0)
    met(0)

    for copy in small[3:]:
        copy.wait()
    values = [kv[i] * (-1.0 / GRID**3) for i in range(32)]

    def look_up(index):
        level = values
        bit = 1
        while len(level) > 1:
            picked = (index & bit) != 0
            level = [
                jnp.where(picked, level[i + 1], level[i]) for i in range(0, len(level), 2)
            ]
            bit *= 2
        return level[0]

    def make_screen(g, carry):
        here = lanes(g, 8)
        left_half = lax.broadcasted_iota(jnp.int32, (8, 128), 1) < GRID

        def chunk(i):
            return classes[here, pl.ds(i * 128, 128)]

        def turned(i):
            return pltpu.roll(chunk(i), GRID, 1)

        for k in range(TILES):
            if k == 0:
                pair = (
                    jnp.where(left_half, chunk(0), turned(16)),
                    jnp.where(left_half, chunk(8), turned(24)),
                )
                screen[here, pl.ds(0, 128)] = look_up(pair[0])
                screen[here, pl.ds(128, 128)] = look_up(pair[1])
                continue
            if k % 2 == 0:
                mixed = jnp.where(left_half, chunk(k // 2), turned((32 - k) // 2))
            else:
                mixed = jnp.where(left_half, turned((k - 1) // 2), chunk((31 - k) // 2))
            found = look_up(mixed)
            screen[here, pl.ds(k * 256, 128)] = found
            screen[here, pl.ds(k * 256 + 128, 128)] = found
        return carry

    for step in (1, 2):
        meet(step)
        lax.fori_loop(4 * step - 4, 4 * step, make_screen, 0)
        met(step)

    def left_pass(value):
        high, low = split(value)
        return dot(left[...], jnp.concatenate([high, high, low], axis=0))

    def right_pass(value, w, w_rest):
        high, low = split(value)
        both = dot(jnp.concatenate([high, low], axis=0), w)
        return both[:GRID] + both[GRID:] + dot(high, w_rest)

    def in_plane(shift):
        j = plane_at(*shift)
        for dx in (2, 1, 3, 0):
            for side in (1, 0):
                if shift != (0, 0) or dx != 0 or side != 0:
                    yield j * 8 + wrap4(x + dx) * 2 + lax.rem(core + side, 2)

    def send_terms(shift):
        for owner in in_plane(shift):
            remote(
                total.at[lax.rem(owner, 8), pl.ds(owner // 8 * 2, 2)],
                grid_term.at[pl.ds(me * 2, 2)],
                many_send.at[1], many_recv.at[1], owner,
            ).start()

    def one_pair(it, after=None):
        last = it == 4
        after = after or {}
        def first_stage(m, c):
            here = lanes(m, 256)
            work[:, here] = left_pass(read(fields, (0,), m) * read(fields, (it,), m))
            return c

        lax.fori_loop(0, 16, first_stage, 0, unroll=True)
        after.get(1, nothing)()

        def second_stage(g, c):
            here = lanes(g, 8)
            re, im = half_spectrum([work[here, pl.ds(n * 128, 128)] for n in range(32)])
            work[here, pl.ds(0, 128)] = re[0]
            work[here, pl.ds(128, 128)] = re[16]
            for k in range(1, 16):
                work[here, pl.ds(k * 256, 128)] = re[k]
                work[here, pl.ds(k * 256 + 128, 128)] = im[k]
            return c

        lax.fori_loop(0, 8, second_stage, 0)
        after.get(2, nothing)()

        def third_stage(k, c):
            here = lanes(k, 256)
            spectrum = right_pass(work[:, here], w_high[k], w_low[k])
            work[:, here] = right_pass(spectrum * screen[:, here], v_high[k], v_low[k])
            return c

        lax.fori_loop(0, 16, third_stage, 0, unroll=True)
        after.get(3, nothing)()

        def fourth_stage(g, c):
            here = lanes(g, 8)
            re = [work[here, pl.ds(0, 128)]]
            im = [None]
            for k in range(1, 16):
                re.append(work[here, pl.ds(k * 256, 128)])
                im.append(work[here, pl.ds(k * 256 + 128, 128)])
            re.append(work[here, pl.ds(128, 128)])
            im.append(None)
            out = half_spectrum_transposed(re, im)
            for n in range(32):
                work[here, pl.ds(n * 128, 128)] = out[n]
            return c

        lax.fori_loop(0, 8, fourth_stage, 0)
        after.get(4, nothing)()

        for start in range(0, 16, SENT_TOGETHER):
            for dz, dy in SHIFTS[start : start + SENT_TOGETHER]:
                j = plane_at(dz, dy)
                added = left_pass(work[:, lanes(j, 256)])
                for i in range(2):
                    part = added[:, i * 128 : i * 128 + 128].reshape(8, 8, 128)
                    term = part * fields[it, :, 2 * j + i]
                    if it == 0:
                        total[:, 2 * j + i] = term
                    else:
                        total[:, 2 * j + i] += term
            if last and start > 0:
                for shift in SHIFTS[start - SENT_TOGETHER : start]:
                    send_terms(shift)

    def next_step(step):
        met(step)
        meet(step + 1)

    def pass_orbital(slot, part, orbital, x_there, side):
        wait_field(slot, part).wait_recv()
        send_near(slot, orbital)
        send_across(slot, orbital, x_there, side)

    meet(3)
    one_pair(
        0,
        {1: lambda: next_step(3), 2: lambda: next_step(4), 3: lambda: next_step(5),
         4: lambda: met(6)},
    )
    to_partner.wait_recv()

    def fetch_second():
        for part in range(2):
            wait_field(2, part).wait_send()
        pl.when(second_crosses)(pass_on)
        pl.when(jnp.logical_not(second_crosses))(lambda: send_field(4, 2, second, core))

    one_pair(
        1,
        {1: fetch_second,
         3: lambda: (
             send_near(0, me),
             pass_orbital(2, 0, second, wrap4(x - 1 + 2 * core), 1 - core),
         )},
    )
    wait_field(2, 1).wait_recv()
    forward_on.start()
    one_pair(2)
    forward_on.wait_recv()
    one_pair(
        3, {4: lambda: pass_orbital(4, 2, first, wrap4(x + 1 - 2 * core), core)}
    )
    wait_field(4, 3).wait_recv()
    one_pair(4)
    for shift in SHIFTS[16 - SENT_TOGETHER :]:
        send_terms(shift)
    grid_term[pl.ds(me * 2, 2)] = total[lax.rem(me, 8), pl.ds(plane * 2, 2)]

    def wait_many(count, buffer, index):
        part = buffer.at[pl.ds(0, count)]
        remote(part, part, many_send.at[index], many_recv.at[index], partner).wait_recv()

    wait_many(125 * 2, grid_orb, 0)
    def across(buffer, s):
        flat = buffer.reshape(BANDS * 16, 128)
        return jnp.concatenate(
            [flat[pl.ds(8 * i + s, BANDS, stride=16), :] for i in range(2)], axis=1
        )

    for s in range(8):
        a_high, a_low = split(across(grid_orb, s))
        orb_high[s], orb_low[s] = a_high, a_low
    wait_many(127 * 2, grid_term, 1)
    result = jnp.zeros((BANDS, BANDS), f32)
    for s in range(8):
        a_high, a_low = orb_high[s], orb_low[s]
        b_high, b_low = split(across(grid_term, s))
        both = dot_t(jnp.concatenate([a_high, a_low], axis=0), b_high)
        result += both[:BANDS] + both[BANDS:] + dot_t(a_high, b_low)
    result = result * (1.0 / GRID**3)
    for i in range(BANDS):
        gram[i] = result[i : i + 1, :]

    for shift in SHIFTS:
        for owner in in_plane(shift):
            remote(
                gram.at[owner], rows.at[me], many_send.at[2], many_recv.at[2], owner
            ).start()
    rows[me] = gram[me]
    part = rows.at[pl.ds(0, BANDS - 1)]
    remote(part, part, many_send.at[2], many_recv.at[2], partner).wait_recv()
    margin[...] = jnp.sum(rows[...], axis=0)

    to_partner.wait_send()
    forward_on.wait_send()
    for part in range(2, 4):
        wait_field(4, part).wait_send()
    passed_on()
    part = grid_orb.at[pl.ds(0, 125 * 2)]
    remote(part, part, many_send.at[0], many_recv.at[0], partner).wait_send()
    part = grid_term.at[pl.ds(0, 127 * 2)]
    remote(part, part, many_send.at[1], many_recv.at[1], partner).wait_send()
    part = rows.at[pl.ds(0, BANDS - 1)]
    remote(part, part, many_send.at[2], many_recv.at[2], partner).wait_send()


def finish(total, margin, exch, out, sem):
    copy = pltpu.make_async_copy(total, exch, sem)
    copy.start()
    out[...] = margin[...]
    copy.wait()


def local(orbitals, kernel_values, shell_index):
    any_space = pl.BlockSpec(memory_space=pl.ANY)
    hbm = pl.BlockSpec(memory_space=pltpu.HBM)
    vmem = pl.BlockSpec(memory_space=pltpu.VMEM)
    tables = constants()
    total, margin = pl.pallas_call(
        kernel,
        out_shape=(pltpu.VMEM(TILED, f32), pltpu.VMEM((1, BANDS), f32)),
        in_specs=[hbm, pl.BlockSpec(memory_space=pltpu.SMEM)] + [hbm] * 5,
        out_specs=(vmem, vmem),
        scratch_shapes=[
            pltpu.VMEM((5, *TILED), f32),
            pltpu.VMEM((GRID, WIDE), f32),
            pltpu.VMEM((GRID, WIDE), f32),
            pltpu.VMEM((GRID, WIDE), jnp.int32),
            *[pltpu.VMEM(t.shape, t.dtype) for t in tables],
            *[pltpu.VMEM((TILES, 256, 256), bf16)] * 4,
            pltpu.VMEM((BANDS * 2, 8, 128), f32),
            pltpu.VMEM((BANDS * 2, 8, 128), f32),
            pltpu.VMEM((BANDS, 1, BANDS), f32),
            pltpu.VMEM((BANDS, 1, BANDS), f32),
            pltpu.VMEM(TILED, f32),
            *[pltpu.VMEM((8, BANDS, 256), bf16)] * 2,
            pltpu.SemaphoreType.DMA((6,)),
            pltpu.SemaphoreType.DMA((2,)),
            pltpu.SemaphoreType.DMA((2,)),
            pltpu.SemaphoreType.DMA((4,)),
            pltpu.SemaphoreType.DMA((4,)),
            pltpu.SemaphoreType.DMA((3,)),
            pltpu.SemaphoreType.DMA((3,)),
            pltpu.SemaphoreType.REGULAR((7,)),
            pltpu.SemaphoreType.DMA,
            pltpu.SemaphoreType.DMA((2,)),
        ],
        compiler_params=pltpu.CompilerParams(
            collective_id=0, has_side_effects=True, vmem_limit_bytes=62 * 1024 * 1024 + 768 * 1024
        ),
        name="exchange",
    )(
        orbitals.reshape(8, 8, 32, 128).transpose(0, 2, 1, 3),
        kernel_values,
        shell_index,
        *[jnp.asarray(c) for c in tables],
    )
    exchange, margin = pl.pallas_call(
        finish,
        out_shape=(
            jax.ShapeDtypeStruct(TILED, f32),
            jax.ShapeDtypeStruct((1, BANDS), f32),
        ),
        in_specs=[vmem, vmem],
        out_specs=(any_space, vmem),
        scratch_shapes=[pltpu.SemaphoreType.DMA],
        name="finish",
    )(
        pltpu.with_memory_space_constraint(total, pltpu.VMEM),
        pltpu.with_memory_space_constraint(margin, pltpu.VMEM),
    )
    return exchange.transpose(0, 2, 1, 3).reshape(1, GRID, WIDE), margin


def solution(mesh):
    return jax.shard_map(
        local,
        mesh=mesh,
        in_specs=(P("band", None, None), P(), P()),
        out_specs=(P("band", None, None), P("band", None)),
        check_vma=False,
    )
```

```python
import math

import jax
import jax.numpy as jnp
import numpy as np
from jax import lax
from jax.experimental import pallas as pl
from jax.experimental.pallas import tpu as pltpu
from jax.sharding import PartitionSpec as P

GRID = 64
WIDE = GRID * GRID
BANDS = 128
TILES = 16
SENT_TOGETHER = 2
TILED = (8, 32, 8, 128)
SHIFTS = sorted(
    ((dz, dy) for dz in range(4) for dy in range(4)),
    key=lambda s: -min(s[0], 4 - s[0]) - min(s[1], 4 - s[1]),
)
MESH = pl.DeviceIdType.MESH
f32 = jnp.float32
bf16 = jnp.bfloat16


def cas(angle):
    return math.cos(angle) + math.sin(angle)


def cas_table():
    index = np.arange(GRID)
    angle = 2.0 * math.pi / GRID * (index[:, None] * index[None] % GRID)
    return np.cos(angle) + np.sin(angle)


def frequencies(k):
    return (0, 32, 16, 48) if k == 0 else (k, 32 - k, 64 - k, 32 + k)


def mixing(k):
    table = np.zeros((4, 4))
    for t, b in enumerate(frequencies(k)):
        for q in range(4):
            part, r = q // 2, q % 2
            angle = 2.0 * math.pi * b * r / GRID
            if k == 0:
                table[q, t] = cas(angle) if (part == 0) == (b % 32 == 0) else 0.0
            elif part == 0:
                table[q, t] = cas(angle)
            else:
                sign = 1.0 if b in (k, 32 + k) else -1.0
                table[q, t] = sign * (math.sin(angle) - math.cos(angle))
    return table


def constants():
    table = cas_table()
    high = table.astype(np.float32).astype(bf16)
    low = (table - high.astype(np.float64)).astype(np.float32).astype(bf16)
    left = np.concatenate([high, low, high], axis=1)
    four = np.tile(table, (1, 4)).astype(np.float32)
    mixes = np.stack([mixing(k) for k in range(TILES)])
    forward = np.repeat(mixes.reshape(TILES * 4, 4), GRID, axis=1).astype(np.float32)
    backward = np.repeat(
        np.swapaxes(mixes, 1, 2).reshape(TILES * 4, 4), GRID, axis=1
    ).astype(np.float32)
    return left, four, forward, backward


def half_spectrum(xs):
    n = len(xs)
    if n == 2:
        return [xs[0] + xs[1], xs[0] - xs[1]], [None, None]
    even_re, even_im = half_spectrum(xs[0::2])
    odd_re, odd_im = half_spectrum(xs[1::2])
    h, q = n // 2, n // 4
    re, im = [None] * (h + 1), [None] * (h + 1)
    re[0], re[h] = even_re[0] + odd_re[0], even_re[0] - odd_re[0]
    for k in range(1, q):
        c, s = math.cos(2 * math.pi * k / n), -math.sin(2 * math.pi * k / n)
        if 2 * k == q:
            t_re, t_im = (odd_re[k] + odd_im[k]) * c, (odd_im[k] - odd_re[k]) * c
        else:
            t_re = odd_re[k] * c - odd_im[k] * s
            t_im = odd_re[k] * s + odd_im[k] * c
        re[k], im[k] = even_re[k] + t_re, even_im[k] + t_im
        re[h - k], im[h - k] = even_re[k] - t_re, t_im - even_im[k]
    re[q], im[q] = even_re[q], -odd_re[q]
    return re, im


def half_spectrum_transposed(re, im):
    h = len(re) - 1
    n = 2 * h
    if n == 2:
        return [re[0] + re[1], re[0] - re[1]]
    q = n // 4
    even_re, even_im = [None] * (q + 1), [None] * (q + 1)
    odd_re, odd_im = [None] * (q + 1), [None] * (q + 1)
    even_re[0], odd_re[0] = re[0] + re[h], re[0] - re[h]
    for k in range(1, q):
        even_re[k], even_im[k] = re[k] + re[h - k], im[k] - im[h - k]
        d_re, d_im = re[k] - re[h - k], im[k] + im[h - k]
        c, s = math.cos(2 * math.pi * k / n), math.sin(2 * math.pi * k / n)
        if 2 * k == q:
            odd_re[k], odd_im[k] = (d_re - d_im) * c, (d_re + d_im) * c
        else:
            odd_re[k], odd_im[k] = d_re * c - d_im * s, d_re * s + d_im * c
    even_re[q], odd_re[q] = re[q], -im[q]
    out = [None] * n
    out[0::2] = half_spectrum_transposed(even_re, even_im)
    out[1::2] = half_spectrum_transposed(odd_re, odd_im)
    return out


def split(x):
    high = x.astype(bf16)
    return high, (x - high.astype(f32)).astype(bf16)


def dot(a, b):
    return jnp.dot(a, b, preferred_element_type=f32)


def dot_t(a, b):
    return lax.dot_general(a, b, (((1,), (1,)), ((), ())), preferred_element_type=f32)


def nothing():
    pass


def lanes(index, size):
    return pl.ds(pl.multiple_of(index * size, size), size)


def remote(src, dst, send, recv, device):
    return pltpu.make_async_remote_copy(
        src_ref=src, dst_ref=dst, send_sem=send, recv_sem=recv,
        device_id=(device,), device_id_type=MESH,
    )


def read(ref, lead, m):
    pieces = [ref[*lead, :, 2 * m + i].reshape(GRID, 128) for i in range(2)]
    return jnp.concatenate(pieces, axis=1)


def kernel(
    orb, kv, shell, left_in, four_in, forward_in, backward_in, total, margin,
    fields, work, screen, classes, left, four, forward, backward,
    w_high, w_low, v_high, v_low, grid_orb, grid_term, gram, rows, relay,
    orb_high, orb_low,
    load_sem, send_sem, recv_sem, part_send, part_recv, many_send, many_recv, meet_sem,
    relay_send, relay_recv,
):
    me = lax.axis_index("band")
    core = lax.rem(me, 2)
    x = lax.rem(me // 2, 4)
    plane = me // 8
    partner = me + 1 - 2 * core
    first = lax.rem(me + BANDS - 2 + 4 * core, BANDS)
    second = lax.rem(me + 2 - 4 * core + BANDS, BANDS)

    def wrap4(v):
        return lax.rem(v + 4, 4)

    def plane_at(dz, dy):
        return wrap4(plane // 4 + dz) * 4 + wrap4(plane + dy)

    load = pltpu.make_async_copy(orb, fields.at[0], load_sem.at[0])
    load.start()

    meetings = [partner]
    neighbours = [first, second, lax.rem(me + 8, BANDS), lax.rem(me + BANDS - 8, BANDS)]
    for scale in (2, 8, 32):
        here = lax.rem(me // scale, 4)
        base = me - here * scale
        meetings.append(me + scale * (1 - 2 * lax.rem(here, 2)))
        meetings.append(base + scale * (3 - here))
    barrier = pltpu.get_barrier_semaphore()
    for device in neighbours + meetings:
        pl.semaphore_signal(barrier, inc=1, device_id=(device,), device_id_type=MESH)
    small = [
        pltpu.make_async_copy(src, dst, load_sem.at[i + 1])
        for i, (src, dst) in enumerate(
            [(four_in, four), (forward_in, forward), (backward_in, backward),
             (left_in, left), (shell, classes)]
        )
    ]
    for copy in small:
        copy.start()
    pl.semaphore_wait(barrier, len(neighbours + meetings))
    load.wait()

    to_partner = remote(fields.at[0], fields.at[1], send_sem.at[0], recv_sem.at[0], partner)
    forward_on = remote(fields.at[2], fields.at[3], send_sem.at[1], recv_sem.at[1], partner)

    def send_groups(source, target, device_x, below, send, recv, part, device):
        start = 2 * device_x - below + 8
        for i in range(8):
            group = lax.rem(start + i, 8)
            index = part if i < 3 else part + 1
            remote(source(i, group), target(i, group), send(index), recv(index), device).start()

    def send_field(slot, part, device, below):
        send_groups(
            lambda i, group: fields.at[0, group], lambda i, group: fields.at[slot, group],
            lax.rem(device // 2, 4), below,
            lambda index: part_send.at[index], lambda index: part_recv.at[index],
            part, device,
        )

    second_crosses = x == 3 - 3 * core

    def send_ahead():
        send_groups(
            lambda i, group: fields.at[0, group], lambda i, group: relay.at[i],
            lax.rem(second // 2, 4), core,
            lambda index: part_send.at[index], lambda index: relay_recv.at[index - 2],
            2, lax.rem(me + 8 - 16 * core + BANDS, BANDS),
        )

    def pass_on():
        up = x // 3
        device = lax.rem(me + 6 - 12 * up + BANDS, BANDS)
        for part, groups in ((0, range(3)), (1, range(3, 8))):
            ref = relay.at[pl.ds(0, len(groups))]
            remote(ref, ref, relay_send, relay_recv.at[part], partner).wait_recv()
            for i in groups:
                remote(
                    relay.at[i],
                    fields.at[4, lax.rem(2 * (3 - 3 * up) - core + 8 + i, 8)],
                    relay_send, part_recv.at[2 + part], device,
                ).start()

    def passed_on():
        @pl.when(second_crosses)
        def _():
            remote(relay, relay, relay_send, relay_recv.at[0], partner).wait_send()

    def wait_field(slot, part):
        count = 3 if part % 2 == 0 else 5
        ref = fields.at[slot, pl.ds(0, count)]
        return remote(ref, ref, part_send.at[part], part_recv.at[part], partner)

    send_field(2, 0, first, 1 - core)
    pl.when(second_crosses)(send_ahead)
    to_partner.start()

    def send_slice(slot, orbital, owner):
        remote(
            fields.at[slot, lax.rem(owner, 8), pl.ds(owner // 8 * 2, 2)],
            grid_orb.at[pl.ds(orbital * 2, 2)],
            many_send.at[0], many_recv.at[0], owner,
        ).start()

    def send_near(slot, orbital):
        def one(t, carry):
            there = lax.rem(plane + t // 2, 16)
            side = lax.rem(core + t, 2)
            send_slice(slot, orbital, there * 8 + x * 2 + side)
            return carry

        lax.fori_loop(1, 32, one, 0)
        grid_orb[pl.ds(orbital * 2, 2)] = fields[slot, lax.rem(me, 8), pl.ds(plane * 2, 2)]

    def send_across(slot, orbital, x_there, side):
        def one(t, carry):
            there = lax.rem(plane + t, 16)
            send_slice(slot, orbital, there * 8 + x_there * 2 + side)
            return carry

        lax.fori_loop(0, 16, one, 0)

    def meet(step):
        pl.semaphore_signal(
            meet_sem.at[step], inc=1, device_id=(meetings[step],), device_id_type=MESH
        )

    def met(step):
        pl.semaphore_wait(meet_sem.at[step], 1)

    def make_tables(k, carry):
        for q in range(4):
            rows_here = pl.ds(q * GRID, GRID)
            high, low = split(four[...] * forward[pl.ds(k * 4 + q, 1), :])
            w_high[k, rows_here, :] = high
            w_low[k, rows_here, :] = low
            high, low = split(four[...] * backward[pl.ds(k * 4 + q, 1), :])
            v_high[k, rows_here, :] = high
            v_low[k, rows_here, :] = low
        return carry

    for copy in small[:3]:
        copy.wait()
    meet(0)
    lax.fori_loop(0, TILES, make_tables, 0)
    met(0)

    for copy in small[3:]:
        copy.wait()
    values = [kv[i] * (-1.0 / GRID**3) for i in range(32)]

    def look_up(index):
        level = values
        bit = 1
        while len(level) > 1:
            picked = (index & bit) != 0
            level = [
                jnp.where(picked, level[i + 1], level[i]) for i in range(0, len(level), 2)
            ]
            bit *= 2
        return level[0]

    def make_screen(g, carry):
        here = lanes(g, 8)
        left_half = lax.broadcasted_iota(jnp.int32, (8, 128), 1) < GRID

        def chunk(i):
            return classes[here, pl.ds(i * 128, 128)]

        def turned(i):
            return pltpu.roll(chunk(i), GRID, 1)

        for k in range(TILES):
            if k == 0:
                pair = (
                    jnp.where(left_half, chunk(0), turned(16)),
                    jnp.where(left_half, chunk(8), turned(24)),
                )
                screen[here, pl.ds(0, 128)] = look_up(pair[0])
                screen[here, pl.ds(128, 128)] = look_up(pair[1])
                continue
            if k % 2 == 0:
                mixed = jnp.where(left_half, chunk(k // 2), turned((32 - k) // 2))
            else:
                mixed = jnp.where(left_half, turned((k - 1) // 2), chunk((31 - k) // 2))
            found = look_up(mixed)
            screen[here, pl.ds(k * 256, 128)] = found
            screen[here, pl.ds(k * 256 + 128, 128)] = found
        return carry

    for step in (1, 2):
        meet(step)
        lax.fori_loop(4 * step - 4, 4 * step, make_screen, 0)
        met(step)

    def left_pass(value):
        high, low = split(value)
        return dot(left[...], jnp.concatenate([high, high, low], axis=0))

    def right_pass(value, w, w_rest):
        high, low = split(value)
        both = dot(jnp.concatenate([high, low], axis=0), w)
        return both[:GRID] + both[GRID:] + dot(high, w_rest)

    def in_plane(shift):
        j = plane_at(*shift)
        for dx in (2, 1, 3, 0):
            for side in (1, 0):
                if shift != (0, 0) or dx != 0 or side != 0:
                    yield j * 8 + wrap4(x + dx) * 2 + lax.rem(core + side, 2)

    def send_terms(shift):
        for owner in in_plane(shift):
            remote(
                total.at[lax.rem(owner, 8), pl.ds(owner // 8 * 2, 2)],
                grid_term.at[pl.ds(me * 2, 2)],
                many_send.at[1], many_recv.at[1], owner,
            ).start()

    def one_pair(it, after=None):
        last = it == 4
        after = after or {}
        def first_stage(m, c):
            here = lanes(m, 256)
            work[:, here] = left_pass(read(fields, (0,), m) * read(fields, (it,), m))
            return c

        lax.fori_loop(0, 16, first_stage, 0, unroll=True)
        after.get(1, nothing)()

        def second_stage(g, c):
            here = lanes(g, 8)
            re, im = half_spectrum([work[here, pl.ds(n * 128, 128)] for n in range(32)])
            work[here, pl.ds(0, 128)] = re[0]
            work[here, pl.ds(128, 128)] = re[16]
            for k in range(1, 16):
                work[here, pl.ds(k * 256, 128)] = re[k]
                work[here, pl.ds(k * 256 + 128, 128)] = im[k]
            return c

        lax.fori_loop(0, 8, second_stage, 0)
        after.get(2, nothing)()

        def third_stage(k, c):
            here = lanes(k, 256)
            spectrum = right_pass(work[:, here], w_high[k], w_low[k])
            work[:, here] = right_pass(spectrum * screen[:, here], v_high[k], v_low[k])
            return c

        lax.fori_loop(0, 16, third_stage, 0, unroll=True)
        after.get(3, nothing)()

        def fourth_stage(g, c):
            here = lanes(g, 8)
            re = [work[here, pl.ds(0, 128)]]
            im = [None]
            for k in range(1, 16):
                re.append(work[here, pl.ds(k * 256, 128)])
                im.append(work[here, pl.ds(k * 256 + 128, 128)])
            re.append(work[here, pl.ds(128, 128)])
            im.append(None)
            out = half_spectrum_transposed(re, im)
            for n in range(32):
                work[here, pl.ds(n * 128, 128)] = out[n]
            return c

        lax.fori_loop(0, 8, fourth_stage, 0)
        after.get(4, nothing)()

        for start in range(0, 16, SENT_TOGETHER):
            for dz, dy in SHIFTS[start : start + SENT_TOGETHER]:
                j = plane_at(dz, dy)
                added = left_pass(work[:, lanes(j, 256)])
                for i in range(2):
                    part = added[:, i * 128 : i * 128 + 128].reshape(8, 8, 128)
                    term = part * fields[it, :, 2 * j + i]
                    if it == 0:
                        total[:, 2 * j + i] = term
                    else:
                        total[:, 2 * j + i] += term
            if last and start > 0:
                for shift in SHIFTS[start - SENT_TOGETHER : start]:
                    send_terms(shift)

    def next_step(step):
        met(step)
        meet(step + 1)

    def pass_orbital(slot, part, orbital, x_there, side):
        wait_field(slot, part).wait_recv()
        send_near(slot, orbital)

    meet(3)
    one_pair(
        0,
        {1: lambda: next_step(3), 2: lambda: next_step(4), 3: lambda: next_step(5),
         4: lambda: met(6)},
    )
    to_partner.wait_recv()

    def fetch_second():
        for part in range(2):
            wait_field(2, part).wait_send()
        pl.when(second_crosses)(pass_on)
        pl.when(jnp.logical_not(second_crosses))(lambda: send_field(4, 2, second, core))

    one_pair(
        1,
        {1: fetch_second,
         3: lambda: (
             send_near(0, me),
             pass_orbital(2, 0, second, wrap4(x - 1 + 2 * core), 1 - core),
         )},
    )
    wait_field(2, 1).wait_recv()
    forward_on.start()
    one_pair(2)
    forward_on.wait_recv()
    one_pair(
        3, {4: lambda: pass_orbital(4, 2, first, wrap4(x + 1 - 2 * core), core)}
    )
    wait_field(4, 3).wait_recv()
    send_across(2, second, wrap4(x - 1 + 2 * core), 1 - core)
    send_across(4, first, wrap4(x + 1 - 2 * core), core)
    one_pair(4)
    for shift in SHIFTS[16 - SENT_TOGETHER :]:
        send_terms(shift)
    grid_term[pl.ds(me * 2, 2)] = total[lax.rem(me, 8), pl.ds(plane * 2, 2)]

    def wait_many(count, buffer, index):
        part = buffer.at[pl.ds(0, count)]
        remote(part, part, many_send.at[index], many_recv.at[index], partner).wait_recv()

    wait_many(125 * 2, grid_orb, 0)
    def across(buffer, s):
        flat = buffer.reshape(BANDS * 16, 128)
        return jnp.concatenate(
            [flat[pl.ds(8 * i + s, BANDS, stride=16), :] for i in range(2)], axis=1
        )

    for s in range(8):
        a_high, a_low = split(across(grid_orb, s))
        orb_high[s], orb_low[s] = a_high, a_low
    wait_many(127 * 2, grid_term, 1)
    result = jnp.zeros((BANDS, BANDS), f32)
    for s in range(8):
        a_high, a_low = orb_high[s], orb_low[s]
        b_high, b_low = split(across(grid_term, s))
        both = dot_t(jnp.concatenate([a_high, a_low], axis=0), b_high)
        result += both[:BANDS] + both[BANDS:] + dot_t(a_high, b_low)
    result = result * (1.0 / GRID**3)
    for i in range(BANDS):
        gram[i] = result[i : i + 1, :]

    for shift in SHIFTS:
        for owner in in_plane(shift):
            remote(
                gram.at[owner], rows.at[me], many_send.at[2], many_recv.at[2], owner
            ).start()
    rows[me] = gram[me]
    part = rows.at[pl.ds(0, BANDS - 1)]
    remote(part, part, many_send.at[2], many_recv.at[2], partner).wait_recv()
    margin[...] = jnp.sum(rows[...], axis=0)

    to_partner.wait_send()
    forward_on.wait_send()
    for part in range(2, 4):
        wait_field(4, part).wait_send()
    passed_on()
    part = grid_orb.at[pl.ds(0, 125 * 2)]
    remote(part, part, many_send.at[0], many_recv.at[0], partner).wait_send()
    part = grid_term.at[pl.ds(0, 127 * 2)]
    remote(part, part, many_send.at[1], many_recv.at[1], partner).wait_send()
    part = rows.at[pl.ds(0, BANDS - 1)]
    remote(part, part, many_send.at[2], many_recv.at[2], partner).wait_send()


def finish(total, margin, exch, out, sem):
    copy = pltpu.make_async_copy(total, exch, sem)
    copy.start()
    out[...] = margin[...]
    copy.wait()


def local(orbitals, kernel_values, shell_index):
    any_space = pl.BlockSpec(memory_space=pl.ANY)
    hbm = pl.BlockSpec(memory_space=pltpu.HBM)
    vmem = pl.BlockSpec(memory_space=pltpu.VMEM)
    tables = constants()
    total, margin = pl.pallas_call(
        kernel,
        out_shape=(pltpu.VMEM(TILED, f32), pltpu.VMEM((1, BANDS), f32)),
        in_specs=[hbm, pl.BlockSpec(memory_space=pltpu.SMEM)] + [hbm] * 5,
        out_specs=(vmem, vmem),
        scratch_shapes=[
            pltpu.VMEM((5, *TILED), f32),
            pltpu.VMEM((GRID, WIDE), f32),
            pltpu.VMEM((GRID, WIDE), f32),
            pltpu.VMEM((GRID, WIDE), jnp.int32),
            *[pltpu.VMEM(t.shape, t.dtype) for t in tables],
            *[pltpu.VMEM((TILES, 256, 256), bf16)] * 4,
            pltpu.VMEM((BANDS * 2, 8, 128), f32),
            pltpu.VMEM((BANDS * 2, 8, 128), f32),
            pltpu.VMEM((BANDS, 1, BANDS), f32),
            pltpu.VMEM((BANDS, 1, BANDS), f32),
            pltpu.VMEM(TILED, f32),
            *[pltpu.VMEM((8, BANDS, 256), bf16)] * 2,
            pltpu.SemaphoreType.DMA((6,)),
            pltpu.SemaphoreType.DMA((2,)),
            pltpu.SemaphoreType.DMA((2,)),
            pltpu.SemaphoreType.DMA((4,)),
            pltpu.SemaphoreType.DMA((4,)),
            pltpu.SemaphoreType.DMA((3,)),
            pltpu.SemaphoreType.DMA((3,)),
            pltpu.SemaphoreType.REGULAR((7,)),
            pltpu.SemaphoreType.DMA,
            pltpu.SemaphoreType.DMA((2,)),
        ],
        compiler_params=pltpu.CompilerParams(
            collective_id=0, has_side_effects=True, vmem_limit_bytes=62 * 1024 * 1024 + 768 * 1024
        ),
        name="exchange",
    )(
        orbitals.reshape(8, 8, 32, 128).transpose(0, 2, 1, 3),
        kernel_values,
        shell_index,
        *[jnp.asarray(c) for c in tables],
    )
    exchange, margin = pl.pallas_call(
        finish,
        out_shape=(
            jax.ShapeDtypeStruct(TILED, f32),
            jax.ShapeDtypeStruct((1, BANDS), f32),
        ),
        in_specs=[vmem, vmem],
        out_specs=(any_space, vmem),
        scratch_shapes=[pltpu.SemaphoreType.DMA],
        name="finish",
    )(
        pltpu.with_memory_space_constraint(total, pltpu.VMEM),
        pltpu.with_memory_space_constraint(margin, pltpu.VMEM),
    )
    return exchange.transpose(0, 2, 1, 3).reshape(1, GRID, WIDE), margin


def solution(mesh):
    return jax.shard_map(
        local,
        mesh=mesh,
        in_specs=(P("band", None, None), P(), P()),
        out_specs=(P("band", None, None), P("band", None)),
        check_vma=False,
    )
```
